128 devices in a mesh: grp: 4 (over z), wave: 32 (over x, y, core).
Axes of the slice: x: 4, y: 4, z: 4, core: 2. Of those that a mesh axis runs over, the one named last changes fastest.
Arguments:
- state: bfloat16 [275, 984320], P(None, ('grp', 'wave')), may hold values from -6 to 6
- held_orders: int32 [640], P(('grp', 'wave')), may hold values from -1 to 383, as said below
- pair_lows: int32 [384], P(('grp', 'wave')), may hold values from 0 to 383, each once
- inverses: bfloat16 [384, 2, 137, 137], P(('grp', 'wave')), may hold values from -2 to 3
- height_operator: bfloat16 [137, 137], replicated, may hold values from -0.5 to 0.5
- pressure_column: bfloat16 [137], replicated, may hold values from -5 to 5
- thermal_response_matrix: bfloat16 [137, 137], replicated, may hold values from -0.5 to 0.5
- mass_row: bfloat16 [137], replicated, may hold values from -0.5 to 0.5
Outputs:
- advanced: bfloat16 [275, 984320], P(None, ('grp', 'wave'))
The draws below stay inside these ranges and needn't reach their ends.
Inputs may be any that keep to these rules, and one draw needn't show every extreme that they name: `held_orders`: each of 0 to 383 appears exactly once, all other entries are -1; some device has all 5 of its slots filled.
All inputs are finite; a program needn't handle non-finite values.
Results may differ from the reference program's by a relative error of at most 0.0052.
Values may be sent and summed in bfloat16 or wider, within the bound.
No kernel may reach another device: no remote copies, remote signals or barrier semaphores. Data moves between devices by JAX's collectives and lax.ppermute only.
A program may use at most 128 MiB of HBM per device.

```python
import jax
import jax.numpy as jnp
from jax import lax

LEVELS = 137
KMAX = 5
HALF = 384
TRUNC = 767
ORDER_SLOTS = 640
WIDTH_SLOT = 1538
COLS = 984320


def draw_held_orders(key, part):
    key_a, key_b, key_c = jax.random.split(jax.random.fold_in(key, 11), 3)
    slot_total = ORDER_SLOTS
    device_total = slot_total // KMAX
    scores = jax.random.permutation(key_a, slot_total).astype(jnp.int32)
    full_device = jax.random.randint(key_b, (), 0, device_total)
    owners = jnp.arange(slot_total, dtype=jnp.int32) // KMAX
    scores = scores - jnp.where(owners == full_device, slot_total, 0).astype(jnp.int32)
    ranking = jnp.argsort(jnp.argsort(scores))
    filled = ranking < HALF
    serial = jnp.cumsum(filled.astype(jnp.int32)) - 1
    orders = jax.random.permutation(key_c, HALF).astype(jnp.int32)
    picked = orders[jnp.clip(serial, 0, HALF - 1)]
    return jnp.where(filled, picked, -1).astype(jnp.int32)


def draw_inverses(key, part):
    key_a, key_b = jax.random.split(jax.random.fold_in(key, 23))
    diagonal = jax.random.uniform(key_a, (HALF, 2, LEVELS), jnp.float32, 0.6, 1.4)
    spread = jnp.clip(jax.random.normal(key_b, (HALF, 2, LEVELS, LEVELS), jnp.float32), -6.0, 6.0) * (0.6 / LEVELS ** 0.5)
    identity = jnp.eye(LEVELS, dtype=jnp.float32)
    return (spread + diagonal[..., None] * identity).astype(jnp.bfloat16)


def levels(rng, dims, pieces, low, top_value):
    level = 1.0
    for dim, parts in pieces:
        draws = jax.random.uniform(jax.random.fold_in(jax.random.fold_in(rng, 6), dim), (parts,), jnp.float32, low / len(pieces), top_value / len(pieces))
        level = level * jnp.repeat(jnp.exp(draws), dims[dim] // parts).reshape((-1,) + (1,) * (len(dims) - 1 - dim))
    return level


def noise(own_key, dims, deviation, most, pieces=(), held_as=jnp.bfloat16):
    loudness = levels(own_key, dims, pieces, -0.22, 0.18) if pieces else 1.0
    drawn = jax.random.normal(own_key, dims, jnp.float32) * deviation * loudness
    return jnp.minimum(jnp.maximum(drawn, -most), most).astype(held_as)


def setup_inputs(seed: int = 0) -> dict:
    splits = jax.random.split(jax.random.key(seed), 9)
    state = noise(splits[0], (2 * LEVELS + 1, COLS), 1.0, 6.0, ((1, 128),))
    held_orders = draw_held_orders(jax.random.fold_in(splits[8], 71), 0)
    pair_lows = jax.random.permutation(splits[2], HALF).astype(jnp.int32)
    inverses = draw_inverses(jax.random.fold_in(splits[8], 71), 0)
    height_operator = noise(splits[4], (LEVELS, LEVELS), LEVELS ** -0.5, 0.5)
    pressure_column = noise(splits[5], (LEVELS,), 1.0, 5.0)
    thermal_response_matrix = noise(splits[6], (LEVELS, LEVELS), LEVELS ** -0.5, 0.5)
    mass_row = noise(splits[7], (LEVELS,), LEVELS ** -0.5, 0.5)
    return {"state": state, "held_orders": held_orders, "pair_lows": pair_lows, "inverses": inverses, "height_operator": height_operator, "pressure_column": pressure_column, "thermal_response_matrix": thermal_response_matrix, "mass_row": mass_row}


def reference(state, held_orders, pair_lows, inverses, height_operator, pressure_column, thermal_response_matrix, mass_row):
    layer_heights_count = LEVELS
    truncation = TRUNC
    slot_width = WIDTH_SLOT
    slot_of = jnp.zeros((HALF,), jnp.int32).at[jnp.where(held_orders >= 0, held_orders, HALF)].set(
        jnp.arange(ORDER_SLOTS, dtype=jnp.int32), mode="drop")
    pair_of = jnp.zeros((HALF,), jnp.int32).at[pair_lows].set(jnp.arange(HALF, dtype=jnp.int32))
    coeff_index = jnp.arange(slot_width // 2, dtype=jnp.int32)
    denom = float(truncation * (truncation + 1))

    def pair_block(low_degree):
        high_degree = truncation - low_degree
        in_low = coeff_index <= low_degree
        degree = jnp.where(in_low, low_degree, high_degree)
        order_of = jnp.where(in_low, coeff_index, coeff_index - low_degree - 1)
        pair_m = jnp.minimum(order_of, truncation - order_of)
        position = jnp.where(order_of == pair_m, degree - order_of, degree + 1)
        first_col = slot_of[pair_m] * slot_width + 2 * position
        spectral_stacks = jnp.stack([first_col, first_col + 1], axis=1).reshape(-1).astype(jnp.int32)
        grouped_arrays = jnp.take(state, spectral_stacks, axis=1)
        divergence = grouped_arrays[:layer_heights_count]
        thermal_state_array = grouped_arrays[layer_heights_count:2 * layer_heights_count]
        pressure = grouped_arrays[2 * layer_heights_count]
        lap_scale = jnp.repeat((degree * (degree + 1)).astype(jnp.float32) / denom, 2)
        height_drive_term = jnp.dot(height_operator, thermal_state_array, preferred_element_type=jnp.float32)
        height_drive_term = height_drive_term + pressure_column.astype(jnp.float32)[:, None] * pressure.astype(jnp.float32)[None, :]
        right_side = (divergence.astype(jnp.float32) + lap_scale[None, :] * height_drive_term).astype(jnp.bfloat16)
        slot_pair = pair_of[low_degree]
        div_low = jnp.dot(inverses[slot_pair, 0], right_side, preferred_element_type=jnp.float32)
        div_high = jnp.dot(inverses[slot_pair, 1], right_side, preferred_element_type=jnp.float32)
        next_spreading_rate = jnp.where(jnp.repeat(in_low, 2)[None, :], div_low, div_high).astype(jnp.bfloat16)
        next_thermal_state = (thermal_state_array.astype(jnp.float32)
                    - jnp.dot(thermal_response_matrix, next_spreading_rate, preferred_element_type=jnp.float32)).astype(jnp.bfloat16)
        surface_mass_next = (pressure.astype(jnp.float32)
                     - jnp.dot(mass_row, next_spreading_rate, preferred_element_type=jnp.float32)).astype(jnp.bfloat16)
        return jnp.concatenate([next_spreading_rate, next_thermal_state, surface_mass_next[None, :]], axis=0), spectral_stacks

    blocks, spectral_stacks = lax.map(pair_block, jnp.arange(HALF, dtype=jnp.int32))
    rows = 2 * layer_heights_count + 1
    flat = jnp.transpose(blocks, (1, 0, 2)).reshape(rows, -1)
    result = jnp.zeros((rows, COLS), jnp.bfloat16)
    return result.at[:, spectral_stacks.reshape(-1)].set(flat)
```

```python
import functools

import jax
import jax.numpy as jnp
import numpy as np
from jax import lax
from jax.experimental import pallas as pl
from jax.experimental.pallas import tpu as pltpu
from jax.sharding import Mesh
from jax.sharding import PartitionSpec as P

GRP_WAVE = ("grp", "wave_0", "wave_1", "wave_2")

LANES = 128
ROWS = 24
FRONT = 768
TILE = 1024
BIG = 1 << 20


def edge_masks(slot_count, edge, shape, row_dim):
    rows = lax.broadcasted_iota(jnp.int32, shape, row_dim)
    lanes = lax.broadcasted_iota(jnp.int32, shape, len(shape) - 1)
    group = rows // 2
    return (lanes >= edge * group) & (lanes < edge * (group + 1)) & (rows < 4 * slot_count + 2)


def parity_fold(parts, axis):
    total = parts[0]
    for part in parts[1:]:
        total = total + part
    total = total + pltpu.roll(total, 2, axis)
    return total + pltpu.roll(total, 4, axis)


def slot_lines(columns, orders_ref, slot_count, slot_width):
    order = jnp.full(columns.shape, -1, jnp.int32)
    place = columns
    for s in range(slot_count):
        inside = (columns >= s * slot_width) & (columns < (s + 1) * slot_width)
        order = jnp.where(inside, orders_ref[s], order)
        place = jnp.where(inside, columns - s * slot_width, place)
    return order, place // 2


def rhs_kernel(
    sizes, orders_ref, state_ref, drive_ref, spread_ref, eye_ref, out_ref, xm, xe, lm, le, um, ue
):
    levels, slot_count, slot_width, truncation = sizes
    half = (truncation + 1) // 2
    step = pl.program_id(0)
    padded = spread_ref.shape[1]
    columns = step * TILE + lax.broadcasted_iota(jnp.int32, (1, TILE), 1)
    order, coeff = slot_lines(columns, orders_ref, slot_count, slot_width)
    degree = jnp.where(coeff <= truncation - order, order + coeff, coeff - 1)
    lap = (degree * (degree + 1)).astype(jnp.float32) / float(truncation * (truncation + 1))
    drive = jnp.dot(drive_ref[...], state_ref[...], preferred_element_type=jnp.float32)
    right = state_ref[:padded, :].astype(jnp.float32) + lap * drive
    right = jnp.where(columns < slot_count * slot_width, right, 0.0).astype(jnp.bfloat16)
    spread = jnp.dot(spread_ref[...], right, preferred_element_type=jnp.float32)
    spread = spread.astype(jnp.bfloat16)
    for k in range(TILE // 256):
        lines = lax.dot_general(
            eye_ref[...],
            spread[:, 256 * k : 256 * (k + 1)],
            (((1,), (1,)), ((), ())),
            preferred_element_type=jnp.float32,
        )
        start = pl.multiple_of(FRONT + step * TILE + 256 * k, 256)
        xm[pl.ds(start, 256), :] = lines[:, :LANES]
        xe[pl.ds(start, 256), :] = lines[:, LANES:]

    @pl.when(step == pl.num_programs(0) - 1)
    def _():
        def regroup(s, carry):
            order = jnp.maximum(orders_ref[s], 0)
            base = FRONT + s * slot_width
            for p in range(2):
                for x, low, up in ((xm, lm, um), (xe, le, ue)):
                    up[pl.ds(2 * s + p, half, stride=ROWS), :] = x[
                        pl.ds(base + 2 * (half + 1) + p, half, stride=2), :
                    ]
                    low[pl.ds(2 * s + p, half, stride=16), :] = x[
                        pl.ds(base - 2 * order + p, half, stride=2), :
                    ]
                    up[pl.ds(2 * (slot_count + s) + p, half, stride=ROWS), :] = x[
                        pl.ds(base + 2 * (half - order) + p, half, stride=2), :
                    ]

                    @pl.when(orders_ref[s] >= 0)
                    def _(x=x, up=up, p=p):
                        third = ROWS * (half - 1 - order) + 4 * slot_count + p
                        up[pl.ds(third, 1), :] = x[
                            pl.ds(base + 2 * (truncation + 1 - order) + p, 1), :
                        ]

            return carry

        lax.fori_loop(0, slot_count, regroup, 0)
        row = lax.broadcasted_iota(jnp.int32, (16, LANES), 0)
        order_rows = jnp.full((16, LANES), BIG, jnp.int32)
        for s in range(slot_count):
            order_rows = jnp.where(row // 2 == s, jnp.maximum(orders_ref[s], 0), order_rows)
        mask = edge_masks(slot_count, levels - LANES, (ROWS, LANES), 0)
        tail = lax.broadcasted_iota(jnp.int32, (8, LANES), 0) >= 6

        def assemble(n, carry):
            start = pl.multiple_of(ROWS * (half - 1 - n), 8)
            low = pl.multiple_of(16 * n, 16)
            body = um[pl.ds(start, ROWS), :]
            edge = ue[pl.ds(start, ROWS), :]
            own = order_rows <= n
            top = jnp.where(own, lm[pl.ds(low, 16), :], body[:16])
            top_edge = jnp.where(own, le[pl.ds(low, 16), :], edge[:16])
            folded = parity_fold(
                [
                    jnp.where(mask[:8], top_edge[:8], 0.0),
                    jnp.where(mask[8:16], top_edge[8:], 0.0),
                    jnp.where(mask[16:], edge[16:], 0.0),
                ],
                0,
            )
            block = jnp.concatenate([top, jnp.where(tail, folded, body[16:])], axis=0)
            out_ref[n] = block.astype(jnp.bfloat16)
            return carry

        lax.fori_loop(0, half, assemble, 0, unroll=4)


def permute_kernel(pair_count, index_ref, blocks_ref, out_ref):
    def body(d, carry):
        for j in range(pair_count):
            out_ref[d * pair_count + j] = blocks_ref[index_ref[d, j]]
        return carry

    lax.fori_loop(0, out_ref.shape[0] // pair_count, body, 0, unroll=4)


def solve_kernel(sizes, lows_ref, blocks_ref, weights_ref, orders_ref, out_ref):
    levels, slot_count = sizes
    count, pair_count = blocks_ref.shape[0], blocks_ref.shape[1]
    shape = (count, ROWS, LANES)
    mask = edge_masks(slot_count, levels - LANES, shape, 1)
    row = lax.broadcasted_iota(jnp.int32, shape, 1)
    for j in range(pair_count):
        body = blocks_ref[:, j].astype(jnp.float32)
        edge = jnp.where(row % 2 == 0, body[:, ROWS - 2 : ROWS - 1], body[:, ROWS - 1 :])
        edge = jnp.where(mask, edge, 0.0)
        lines = jnp.concatenate([body, edge], axis=-1).reshape(count * ROWS, 2 * LANES)
        lines = lines.astype(jnp.bfloat16)
        upper = jnp.dot(lines, weights_ref[j, 1], preferred_element_type=jnp.float32)
        lower = jnp.dot(lines, weights_ref[j, 0], preferred_element_type=jnp.float32)
        own = orders_ref[...] <= lows_ref[j]
        main = jnp.where(own, lower[:, :LANES], upper[:, :LANES]).reshape(shape)
        edge = jnp.where(own, lower[:, LANES:], upper[:, LANES:]).reshape(shape)
        edge = jnp.where(mask, edge, 0.0)
        folded = parity_fold([edge[:, :8], edge[:, 8:16], edge[:, 16:]], 1)
        folded = jnp.concatenate([folded, folded, folded], axis=1)
        out_ref[:, j] = jnp.where(row >= ROWS - 2, folded, main).astype(jnp.bfloat16)


def final_kernel(
    sizes, index_ref, orders_ref, blocks_ref, state_ref, weights_ref, out_ref, xm, xe, lm, le, um, ue
):
    levels, slot_count, slot_width, truncation, pair_count = sizes
    half = (truncation + 1) // 2
    step = pl.program_id(0)

    @pl.when(step == 0)
    def _():
        mask = edge_masks(slot_count, levels - LANES, (ROWS, LANES), 0)
        even = lax.broadcasted_iota(jnp.int32, (ROWS, LANES), 0) % 2 == 0

        def unfold(d, carry):
            for j in range(pair_count):
                n = index_ref[d, j]
                body = blocks_ref[d * pair_count + j].astype(jnp.float32)
                edge = jnp.where(even, body[ROWS - 2 : ROWS - 1], body[ROWS - 1 :])
                edge = jnp.where(mask, edge, 0.0)
                start = pl.multiple_of(ROWS * (half - 1 - n), 8)
                low = pl.multiple_of(16 * n, 16)
                um[pl.ds(start, ROWS), :] = body
                ue[pl.ds(start, ROWS), :] = edge
                lm[pl.ds(low, 16), :] = body[:16]
                le[pl.ds(low, 16), :] = edge[:16]
            return carry

        lax.fori_loop(0, half // pair_count, unfold, 0, unroll=2)

        def regroup(k, carry):
            s = slot_count - 1 - k
            order = jnp.maximum(orders_ref[s], 0)
            base = FRONT + s * slot_width
            for p in range(2):
                for x, low, up in ((xm, lm, um), (xe, le, ue)):
                    x[pl.ds(base + 2 * (half + 1) + p, half, stride=2), :] = up[
                        pl.ds(2 * s + p, half, stride=ROWS), :
                    ]
                    x[pl.ds(base - 2 * order + p, half, stride=2), :] = low[
                        pl.ds(2 * s + p, half, stride=16), :
                    ]
                    x[pl.ds(base + 2 * (half - order) + p, half, stride=2), :] = up[
                        pl.ds(2 * (slot_count + s) + p, half, stride=ROWS), :
                    ]
                third = ROWS * (half - 1 - order) + 4 * slot_count + p
                place = base + 2 * (truncation + 1 - order) + p
                xm[pl.ds(place, 1), :] = um[pl.ds(third, 1), :]
                xe[pl.ds(place, 1), :] = ue[pl.ds(third, 1), :]
            return carry

        lax.fori_loop(0, slot_count, regroup, 0)

    start = pl.multiple_of(FRONT + step * TILE, 256)
    lines = jnp.concatenate([xm[pl.ds(start, TILE), :], xe[pl.ds(start, TILE), :]], axis=1)
    moved = lax.dot_general(
        weights_ref[...],
        lines.astype(jnp.bfloat16),
        (((1,), (1,)), ((), ())),
        preferred_element_type=jnp.float32,
    )
    columns = step * TILE + lax.broadcasted_iota(jnp.int32, (1, TILE), 1)
    order, _ = slot_lines(columns, orders_ref, slot_count, slot_width)
    kept = lax.broadcasted_iota(jnp.int32, (state_ref.shape[0], 1), 0) >= levels
    base = jnp.where(kept, state_ref[...].astype(jnp.float32), 0.0)
    out_ref[...] = jnp.where(order >= 0, base + moved, 0.0).astype(jnp.bfloat16)


def level_of_lane(levels, slot_count):
    edge = levels - LANES
    table = np.zeros((2 * LANES, levels), np.float32)
    table[np.arange(LANES), np.arange(LANES)] = 1.0
    folded = np.arange(edge * (2 * slot_count + 1))
    table[LANES + folded, LANES + folded % edge] = 1.0
    return table


def shards(
    state,
    held_orders,
    pair_lows,
    inverses,
    height_operator,
    pressure_column,
    thermal_response_matrix,
    mass_row,
):
    levels = height_operator.shape[0]
    pair_count = pair_lows.shape[0]
    slot_count = held_orders.shape[0]
    devices = lax.axis_size(GRP_WAVE)
    half = pair_count * devices
    truncation = 2 * half - 1
    slot_width = 2 * (truncation + 2)
    width = slot_count * slot_width
    rows = state.shape[0]
    steps = -(-width // TILE)
    bf16, f32 = jnp.bfloat16, jnp.float32
    vmem = pl.BlockSpec(memory_space=pltpu.VMEM)
    smem = pl.BlockSpec(memory_space=pltpu.SMEM)
    params = functools.partial(pltpu.CompilerParams, vmem_limit_bytes=56 * 1024 * 1024)
    scratch = [
        pltpu.VMEM((FRONT + steps * TILE, LANES), f32),
        pltpu.VMEM((FRONT + steps * TILE, LANES), f32),
        pltpu.VMEM((16 * half, LANES), f32),
        pltpu.VMEM((16 * half, LANES), f32),
        pltpu.VMEM((ROWS * half, LANES), f32),
        pltpu.VMEM((ROWS * half, LANES), f32),
    ]

    own = jnp.concatenate([pair_lows, held_orders])
    own = jnp.pad(own, (0, LANES - own.shape[0]))
    index = lax.all_to_all(
        jnp.broadcast_to(own[None, None], (devices, 1, LANES)), GRP_WAVE, 0, 0, tiled=True
    ).reshape(devices, LANES)

    table = jnp.asarray(level_of_lane(levels, slot_count), bf16)
    padded = -(-levels // 16) * 16
    drive = jnp.concatenate(
        [jnp.zeros((levels, levels), bf16), height_operator, pressure_column[:, None]], axis=1
    )
    drive = jnp.pad(drive, ((0, padded - levels), (0, 0)))
    spread = jnp.pad(table, ((0, 0), (0, padded - levels)))
    eye = jnp.eye(256, dtype=bf16)

    blocks = pl.pallas_call(
        functools.partial(rhs_kernel, (levels, slot_count, slot_width, truncation)),
        grid=(steps,),
        in_specs=[
            smem,
            pl.BlockSpec((rows, TILE), lambda i: (0, i)),
            vmem,
            vmem,
            vmem,
        ],
        out_specs=pl.BlockSpec((half, ROWS, LANES), lambda i: (0, 0, 0)),
        out_shape=jax.ShapeDtypeStruct((half, ROWS, LANES), bf16),
        scratch_shapes=scratch,
        compiler_params=params(),
        cost_estimate=pl.CostEstimate(
            flops=4_000_000_000, bytes_accessed=7_000_000, transcendentals=0
        ),
        name="right_side",
    )(held_orders, state, drive, spread, eye)

    message = pl.pallas_call(
        functools.partial(permute_kernel, pair_count),
        in_specs=[smem, vmem],
        out_specs=vmem,
        out_shape=jax.ShapeDtypeStruct((half, ROWS, LANES), bf16),
        compiler_params=params(),
        name="by_owner",
    )(index, blocks)

    arrived = lax.all_to_all(
        message.reshape(devices, pair_count * ROWS, LANES), GRP_WAVE, 0, 0, tiled=True
    ).reshape(devices, pair_count, ROWS, LANES)

    weights = jnp.einsum("al,jtkl->jtak", table, inverses, preferred_element_type=f32)
    weights = jnp.einsum("jtak,bk->jtab", weights.astype(bf16), table, preferred_element_type=f32)
    weights = weights.astype(bf16)
    all_orders = index[:, pair_count : pair_count + slot_count]
    order_rows = jnp.pad(
        jnp.repeat(all_orders, 2, axis=1),
        ((0, 0), (0, ROWS - 2 * slot_count)),
        constant_values=BIG,
    ).reshape(devices * ROWS, 1)
    order_rows = jnp.broadcast_to(order_rows, (devices * ROWS, LANES))
    chunk = 16
    solved = pl.pallas_call(
        functools.partial(solve_kernel, (levels, slot_count)),
        grid=(devices // chunk,),
        in_specs=[
            smem,
            pl.BlockSpec((chunk, pair_count, ROWS, LANES), lambda i: (i, 0, 0, 0)),
            vmem,
            pl.BlockSpec((chunk * ROWS, LANES), lambda i: (i, 0)),
        ],
        out_specs=pl.BlockSpec((chunk, pair_count, ROWS, LANES), lambda i: (i, 0, 0, 0)),
        out_shape=jax.ShapeDtypeStruct((devices, pair_count, ROWS, LANES), bf16),
        compiler_params=params(),
        name="solve",
    )(pair_lows, arrived, weights, order_rows)

    returned = lax.all_to_all(
        solved.reshape(devices, pair_count * ROWS, LANES), GRP_WAVE, 0, 0, tiled=True
    ).reshape(half, ROWS, LANES)

    response = jnp.concatenate(
        [jnp.eye(levels, dtype=bf16), -thermal_response_matrix, -mass_row[None, :]], axis=0
    )
    response = jnp.dot(response, table.T, preferred_element_type=f32).astype(bf16)
    return pl.pallas_call(
        functools.partial(final_kernel, (levels, slot_count, slot_width, truncation, pair_count)),
        grid=(steps,),
        in_specs=[
            smem,
            smem,
            vmem,
            pl.BlockSpec((rows, TILE), lambda i: (0, i)),
            vmem,
        ],
        out_specs=pl.BlockSpec((rows, TILE), lambda i: (0, i)),
        out_shape=jax.ShapeDtypeStruct((rows, width), bf16),
        scratch_shapes=scratch,
        compiler_params=params(),
        name="final",
    )(index, held_orders, returned, state, response)


def solution(mesh):
    torus = Mesh(
        mesh.devices.reshape(mesh.shape["grp"], 4, 4, 2), ("grp", "wave_0", "wave_1", "wave_2")
    )
    placed = (
        P(None, GRP_WAVE),
        P(GRP_WAVE),
        P(GRP_WAVE),
        P(GRP_WAVE, None, None, None),
        P(),
        P(),
        P(),
        P(),
    )
    return jax.shard_map(
        shards, mesh=torus, in_specs=placed, out_specs=P(None, GRP_WAVE), check_vma=False
    )
```

```python
import functools

import jax
import jax.numpy as jnp
import numpy as np
from jax import lax
from jax.experimental import pallas as pl
from jax.experimental.pallas import tpu as pltpu
from jax.sharding import Mesh
from jax.sharding import PartitionSpec as P

GRP_WAVE = ("grp", "wave_0", "wave_1", "wave_2")

LANES = 128
ROWS = 24
FRONT = 768
TILE = 1024
BIG = 1 << 20
LOW = 17
UP = 25


def edge_masks(slot_count, edge, shape, row_dim):
    rows = lax.broadcasted_iota(jnp.int32, shape, row_dim)
    lanes = lax.broadcasted_iota(jnp.int32, shape, len(shape) - 1)
    group = rows // 2
    return (lanes >= edge * group) & (lanes < edge * (group + 1)) & (rows < 4 * slot_count + 2)


def parity_fold(parts, axis):
    total = parts[0]
    for part in parts[1:]:
        total = total + part
    total = total + pltpu.roll(total, 2, axis)
    return total + pltpu.roll(total, 4, axis)


def slot_lines(columns, orders_ref, slot_count, slot_width):
    order = jnp.full(columns.shape, -1, jnp.int32)
    place = columns
    for s in range(slot_count):
        inside = (columns >= s * slot_width) & (columns < (s + 1) * slot_width)
        order = jnp.where(inside, orders_ref[s], order)
        place = jnp.where(inside, columns - s * slot_width, place)
    return order, place // 2


def rhs_kernel(
    sizes,
    index_ref,
    orders_ref,
    state_ref,
    height_ref,
    pressure_ref,
    place_ref,
    spread_ref,
    eye_ref,
    out_ref,
    drive,
    xm,
    xe,
    lm,
    le,
    um,
    ue,
):
    levels, slot_count, slot_width, truncation, pair_count = sizes
    half = (truncation + 1) // 2
    step = pl.program_id(0)
    padded = spread_ref.shape[1]

    @pl.when(step == 0)
    def _():
        moved = jnp.dot(height_ref[...], place_ref[...], preferred_element_type=jnp.float32)
        row = jnp.broadcast_to(pressure_ref[...].reshape(1, levels), (LANES, levels))
        column = lax.dot_general(
            eye_ref[:levels, :levels], row, (((1,), (1,)), ((), ())),
            preferred_element_type=jnp.float32,
        )
        last = lax.broadcasted_iota(jnp.int32, moved.shape, 1) == 2 * levels
        moved = jnp.where(last, column[:, :1], moved).astype(jnp.bfloat16)
        drive[...] = jnp.zeros_like(drive)
        drive[:levels, :] = moved

    columns = step * TILE + lax.broadcasted_iota(jnp.int32, (1, TILE), 1)
    order, coeff = slot_lines(columns, orders_ref, slot_count, slot_width)
    degree = jnp.where(coeff <= truncation - order, order + coeff, coeff - 1)
    lap = (degree * (degree + 1)).astype(jnp.float32) / float(truncation * (truncation + 1))
    pull = jnp.dot(drive[...], state_ref[...], preferred_element_type=jnp.float32)
    right = state_ref[:padded, :].astype(jnp.float32) + lap * pull
    right = jnp.where(columns < slot_count * slot_width, right, 0.0).astype(jnp.bfloat16)
    spread = jnp.dot(spread_ref[...], right, preferred_element_type=jnp.float32)
    spread = spread.astype(jnp.bfloat16)
    for k in range(TILE // 256):
        lines = lax.dot_general(
            eye_ref[...],
            spread[:, 256 * k : 256 * (k + 1)],
            (((1,), (1,)), ((), ())),
            preferred_element_type=jnp.float32,
        )
        start = pl.multiple_of(FRONT + step * TILE + 256 * k, 256)
        xm[pl.ds(start, 256), :] = lines[:, :LANES]
        xe[pl.ds(start, 256), :] = lines[:, LANES:]

    @pl.when(step == pl.num_programs(0) - 1)
    def _():
        def regroup(s, carry):
            order = jnp.maximum(orders_ref[s], 0)
            base = FRONT + s * slot_width
            for p in range(2):
                for x, low, up in ((xm, lm, um), (xe, le, ue)):
                    up[pl.ds(2 * s + p, half, stride=UP), :] = x[
                        pl.ds(base + 2 * (half + 1) + p, half, stride=2), :
                    ]
                    low[pl.ds(2 * s + p, half, stride=LOW), :] = x[
                        pl.ds(base - 2 * order + p, half, stride=2), :
                    ]
                    up[pl.ds(2 * (slot_count + s) + p, half, stride=UP), :] = x[
                        pl.ds(base + 2 * (half - order) + p, half, stride=2), :
                    ]

                    @pl.when(orders_ref[s] >= 0)
                    def _(x=x, up=up, p=p):
                        third = UP * (half - 1 - order) + 4 * slot_count + p
                        up[pl.ds(third, 1), :] = x[
                            pl.ds(base + 2 * (truncation + 1 - order) + p, 1), :
                        ]

            return carry

        lax.fori_loop(0, slot_count, regroup, 0)
        row = lax.broadcasted_iota(jnp.int32, (16, LANES), 0)
        order_rows = jnp.full((16, LANES), BIG, jnp.int32)
        for s in range(slot_count):
            order_rows = jnp.where(row // 2 == s, jnp.maximum(orders_ref[s], 0), order_rows)
        mask = edge_masks(slot_count, levels - LANES, (ROWS, LANES), 0)
        tail = lax.broadcasted_iota(jnp.int32, (8, LANES), 0) >= 6

        def assemble(d, j):
            n = index_ref[d, j]
            start = UP * (half - 1 - n)
            low = LOW * n
            body = um[pl.ds(start, ROWS), :]
            edge = ue[pl.ds(start, ROWS), :]
            own = order_rows <= n
            top = jnp.where(own, lm[pl.ds(low, 16), :], body[:16])
            top_edge = jnp.where(own, le[pl.ds(low, 16), :], edge[:16])
            folded = parity_fold(
                [
                    jnp.where(mask[:8], top_edge[:8], 0.0),
                    jnp.where(mask[8:16], top_edge[8:], 0.0),
                    jnp.where(mask[16:], edge[16:], 0.0),
                ],
                0,
            )
            block = jnp.concatenate([top, jnp.where(tail, folded, body[16:])], axis=0)
            out_ref[d * pair_count + j] = block.astype(jnp.bfloat16)

        def assemble_all(d, carry):
            for j in range(pair_count):
                assemble(d, j)
            return carry

        lax.fori_loop(0, half // pair_count, assemble_all, 0, unroll=2)


def solve_kernel(sizes, lows_ref, index_ref, blocks_ref, weights_ref, out_ref):
    levels, slot_count = sizes
    count, pair_count = blocks_ref.shape[0], blocks_ref.shape[1]
    shape = (count, ROWS, LANES)
    mask = edge_masks(slot_count, levels - LANES, shape, 1)
    row = lax.broadcasted_iota(jnp.int32, shape, 1)
    slot = lax.broadcasted_iota(jnp.int32, (ROWS, LANES), 0) // 2
    orders = []
    for k in range(count):
        lines = jnp.full((ROWS, LANES), BIG, jnp.int32)
        for s in range(slot_count):
            order = index_ref[pl.program_id(0) * count + k, pair_count + s]
            lines = jnp.where(slot == s, order, lines)
        orders.append(lines)
    orders = jnp.concatenate(orders, axis=0)
    for j in range(pair_count):
        body = blocks_ref[:, j].astype(jnp.float32)
        edge = jnp.where(row % 2 == 0, body[:, ROWS - 2 : ROWS - 1], body[:, ROWS - 1 :])
        edge = jnp.where(mask, edge, 0.0)
        lines = jnp.concatenate([body, edge], axis=-1).reshape(count * ROWS, 2 * LANES)
        lines = lines.astype(jnp.bfloat16)
        upper = jnp.dot(lines, weights_ref[j, 1], preferred_element_type=jnp.float32)
        lower = jnp.dot(lines, weights_ref[j, 0], preferred_element_type=jnp.float32)
        own = orders <= lows_ref[j]
        main = jnp.where(own, lower[:, :LANES], upper[:, :LANES]).reshape(shape)
        edge = jnp.where(own, lower[:, LANES:], upper[:, LANES:]).reshape(shape)
        edge = jnp.where(mask, edge, 0.0)
        folded = parity_fold([edge[:, :8], edge[:, 8:16], edge[:, 16:]], 1)
        folded = jnp.concatenate([folded, folded, folded], axis=1)
        out_ref[:, j] = jnp.where(row >= ROWS - 2, folded, main).astype(jnp.bfloat16)


def final_kernel(
    sizes, index_ref, orders_ref, blocks_ref, state_ref, weights_ref, out_ref, xm, xe, lm, le, um, ue
):
    levels, slot_count, slot_width, truncation, pair_count = sizes
    half = (truncation + 1) // 2
    step = pl.program_id(0)

    @pl.when(step == 0)
    def _():
        mask = edge_masks(slot_count, levels - LANES, (ROWS, LANES), 0)
        even = lax.broadcasted_iota(jnp.int32, (ROWS, LANES), 0) % 2 == 0

        def unfold(d, carry):
            for j in range(pair_count):
                n = index_ref[d, j]
                body = blocks_ref[d * pair_count + j].astype(jnp.float32)
                edge = jnp.where(even, body[ROWS - 2 : ROWS - 1], body[ROWS - 1 :])
                edge = jnp.where(mask, edge, 0.0)
                start = UP * (half - 1 - n)
                low = LOW * n
                um[pl.ds(start, ROWS), :] = body
                ue[pl.ds(start, ROWS), :] = edge
                lm[pl.ds(low, 16), :] = body[:16]
                le[pl.ds(low, 16), :] = edge[:16]
            return carry

        lax.fori_loop(0, half // pair_count, unfold, 0, unroll=2)

        def regroup(k, carry):
            s = slot_count - 1 - k
            order = jnp.maximum(orders_ref[s], 0)
            base = FRONT + s * slot_width
            for p in range(2):
                for x, low, up in ((xm, lm, um), (xe, le, ue)):
                    x[pl.ds(base + 2 * (half + 1) + p, half, stride=2), :] = up[
                        pl.ds(2 * s + p, half, stride=UP), :
                    ]
                    x[pl.ds(base - 2 * order + p, half, stride=2), :] = low[
                        pl.ds(2 * s + p, half, stride=LOW), :
                    ]
                    x[pl.ds(base + 2 * (half - order) + p, half, stride=2), :] = up[
                        pl.ds(2 * (slot_count + s) + p, half, stride=UP), :
                    ]
                third = UP * (half - 1 - order) + 4 * slot_count + p
                place = base + 2 * (truncation + 1 - order) + p
                xm[pl.ds(place, 1), :] = um[pl.ds(third, 1), :]
                xe[pl.ds(place, 1), :] = ue[pl.ds(third, 1), :]
            return carry

        lax.fori_loop(0, slot_count, regroup, 0)

    start = pl.multiple_of(FRONT + step * TILE, 256)
    lines = jnp.concatenate([xm[pl.ds(start, TILE), :], xe[pl.ds(start, TILE), :]], axis=1)
    moved = lax.dot_general(
        weights_ref[...],
        lines.astype(jnp.bfloat16),
        (((1,), (1,)), ((), ())),
        preferred_element_type=jnp.float32,
    )
    columns = step * TILE + lax.broadcasted_iota(jnp.int32, (1, TILE), 1)
    order, _ = slot_lines(columns, orders_ref, slot_count, slot_width)
    kept = lax.broadcasted_iota(jnp.int32, (state_ref.shape[0], 1), 0) >= levels
    base = jnp.where(kept, state_ref[...].astype(jnp.float32), 0.0)
    out_ref[...] = jnp.where(order >= 0, base + moved, 0.0).astype(jnp.bfloat16)


def level_of_lane(levels, slot_count):
    edge = levels - LANES
    table = np.zeros((2 * LANES, levels), np.float32)
    table[np.arange(LANES), np.arange(LANES)] = 1.0
    folded = np.arange(edge * (2 * slot_count + 1))
    table[LANES + folded, LANES + folded % edge] = 1.0
    return table


def shards(
    state,
    held_orders,
    pair_lows,
    inverses,
    height_operator,
    pressure_column,
    thermal_response_matrix,
    mass_row,
):
    levels = height_operator.shape[0]
    pair_count = pair_lows.shape[0]
    slot_count = held_orders.shape[0]
    devices = lax.axis_size(GRP_WAVE)
    half = pair_count * devices
    truncation = 2 * half - 1
    slot_width = 2 * (truncation + 2)
    width = slot_count * slot_width
    rows = state.shape[0]
    steps = -(-width // TILE)
    bf16, f32 = jnp.bfloat16, jnp.float32
    vmem = pl.BlockSpec(memory_space=pltpu.VMEM)
    smem = pl.BlockSpec(memory_space=pltpu.SMEM)

    def params(mib):
        return pltpu.CompilerParams(vmem_limit_bytes=mib * 1024 * 1024)

    scratch = [
        pltpu.VMEM((FRONT + steps * TILE, LANES), f32),
        pltpu.VMEM((FRONT + steps * TILE, LANES), f32),
        pltpu.VMEM((LOW * half, LANES), f32),
        pltpu.VMEM((LOW * half, LANES), f32),
        pltpu.VMEM((UP * half, LANES), f32),
        pltpu.VMEM((UP * half, LANES), f32),
    ]

    own = jnp.concatenate([pair_lows, held_orders])
    own = jnp.pad(own, (0, LANES - own.shape[0]))
    index = lax.all_to_all(
        jnp.broadcast_to(own[None, None], (devices, 1, LANES)), GRP_WAVE, 0, 0, tiled=True
    ).reshape(devices, LANES)

    table = level_of_lane(levels, slot_count)
    padded = -(-levels // 16) * 16
    spread = np.zeros((2 * LANES, padded), np.float32)
    spread[:, :levels] = table
    place = np.zeros((levels, rows), np.float32)
    place[:, levels : 2 * levels] = np.eye(levels)
    table, spread, place = (jnp.asarray(x, bf16) for x in (table, spread, place))
    eye = jnp.asarray(np.eye(256), bf16)

    message = pl.pallas_call(
        functools.partial(rhs_kernel, (levels, slot_count, slot_width, truncation, pair_count)),
        grid=(steps,),
        in_specs=[
            smem,
            smem,
            pl.BlockSpec((rows, TILE), lambda i: (0, i)),
            vmem,
            vmem,
            vmem,
            vmem,
            vmem,
        ],
        out_specs=pl.BlockSpec((half, ROWS, LANES), lambda i: (0, 0, 0)),
        out_shape=jax.ShapeDtypeStruct((half, ROWS, LANES), bf16),
        scratch_shapes=[pltpu.VMEM((padded, rows), bf16)] + scratch,
        compiler_params=params(56),
        name="right_side",
    )(index, held_orders, state, height_operator, pressure_column, place, spread, eye)

    arrived = lax.all_to_all(
        message.reshape(devices, pair_count * ROWS, LANES), GRP_WAVE, 0, 0, tiled=True
    ).reshape(devices, pair_count, ROWS, LANES)

    weights = jnp.einsum("al,jtkl->jtak", table, inverses, preferred_element_type=f32)
    weights = jnp.einsum("jtak,bk->jtab", weights.astype(bf16), table, preferred_element_type=f32)
    weights = weights.astype(bf16)
    chunk = 16
    solved = pl.pallas_call(
        functools.partial(solve_kernel, (levels, slot_count)),
        grid=(devices // chunk,),
        in_specs=[
            smem,
            smem,
            pl.BlockSpec((chunk, pair_count, ROWS, LANES), lambda i: (i, 0, 0, 0)),
            vmem,
        ],
        out_specs=pl.BlockSpec((chunk, pair_count, ROWS, LANES), lambda i: (i, 0, 0, 0)),
        out_shape=jax.ShapeDtypeStruct((devices, pair_count, ROWS, LANES), bf16),
        compiler_params=params(54),
        name="solve",
    )(pair_lows, index, arrived, weights)

    returned = lax.all_to_all(
        solved.reshape(devices, pair_count * ROWS, LANES), GRP_WAVE, 0, 0, tiled=True
    ).reshape(half, ROWS, LANES)

    response = jnp.concatenate(
        [jnp.eye(levels, dtype=bf16), -thermal_response_matrix, -mass_row[None, :]], axis=0
    )
    response = jnp.dot(response, table.T, preferred_element_type=f32).astype(bf16)
    return pl.pallas_call(
        functools.partial(final_kernel, (levels, slot_count, slot_width, truncation, pair_count)),
        grid=(steps,),
        in_specs=[
            smem,
            smem,
            vmem,
            pl.BlockSpec((rows, TILE), lambda i: (0, i)),
            vmem,
        ],
        out_specs=pl.BlockSpec((rows, TILE), lambda i: (0, i)),
        out_shape=jax.ShapeDtypeStruct((rows, width), bf16),
        scratch_shapes=scratch,
        compiler_params=params(48),
        name="final",
    )(index, held_orders, returned, state, response)


def solution(mesh):
    torus = Mesh(
        mesh.devices.reshape(mesh.shape["grp"], 4, 4, 2), ("grp", "wave_0", "wave_1", "wave_2")
    )
    placed = (
        P(None, GRP_WAVE),
        P(GRP_WAVE),
        P(GRP_WAVE),
        P(GRP_WAVE, None, None, None),
        P(),
        P(),
        P(),
        P(),
    )
    return jax.shard_map(
        shards, mesh=torus, in_specs=placed, out_specs=P(None, GRP_WAVE), check_vma=False
    )
```

```python
import functools

import jax
import jax.numpy as jnp
import numpy as np
from jax import lax
from jax.experimental import pallas as pl
from jax.experimental.pallas import tpu as pltpu
from jax.sharding import Mesh
from jax.sharding import PartitionSpec as P

GRP_WAVE = ("grp", "wave_0", "wave_1", "wave_2")

LANES = 128
ROWS = 24
FRONT = 768
TILE = 1024
BIG = 1 << 20
LOW = 17
UP = 25


def edge_masks(slot_count, edge, shape, row_dim):
    rows = lax.broadcasted_iota(jnp.int32, shape, row_dim)
    lanes = lax.broadcasted_iota(jnp.int32, shape, len(shape) - 1)
    group = rows // 2
    return (lanes >= edge * group) & (lanes < edge * (group + 1)) & (rows < 4 * slot_count + 2)


def parity_fold(parts, axis):
    total = parts[0]
    for part in parts[1:]:
        total = total + part
    total = total + pltpu.roll(total, 2, axis)
    return total + pltpu.roll(total, 4, axis)


def slot_lines(columns, orders_ref, slot_count, slot_width):
    order = jnp.full(columns.shape, -1, jnp.int32)
    place = columns
    for s in range(slot_count):
        inside = (columns >= s * slot_width) & (columns < (s + 1) * slot_width)
        order = jnp.where(inside, orders_ref[s], order)
        place = jnp.where(inside, columns - s * slot_width, place)
    return order, place // 2


def rhs_kernel(
    sizes,
    index_ref,
    orders_ref,
    state_ref,
    height_ref,
    pressure_ref,
    place_ref,
    spread_ref,
    eye_ref,
    out_ref,
    drive,
    xm,
    xe,
    lm,
    le,
    um,
    ue,
):
    levels, slot_count, slot_width, truncation, pair_count, streams = sizes
    half = (truncation + 1) // 2
    step = pl.program_id(0)

    @pl.when(step == 0)
    def _():
        moved = jnp.dot(height_ref[...], place_ref[...], preferred_element_type=jnp.float32)
        row = jnp.broadcast_to(pressure_ref[...].reshape(1, levels), (LANES, levels))
        column = lax.dot_general(
            eye_ref[:levels, :levels],
            row,
            (((1,), (1,)), ((), ())),
            preferred_element_type=jnp.float32,
        )
        last = lax.broadcasted_iota(jnp.int32, moved.shape, 1) == moved.shape[1] - 1
        moved = jnp.where(last, column[:, :1], moved).astype(jnp.bfloat16)
        drive[...] = jnp.zeros_like(drive)
        drive[:levels, :] = moved

    @pl.when(step < streams)
    def _():
        columns = step * TILE + lax.broadcasted_iota(jnp.int32, (1, TILE), 1)
        order, coeff = slot_lines(columns, orders_ref, slot_count, slot_width)
        degree = jnp.where(coeff <= truncation - order, order + coeff, coeff - 1)
        lap = (degree * (degree + 1)).astype(jnp.float32) / float(truncation * (truncation + 1))
        padded = drive.shape[0]
        pull = jnp.dot(drive[...], state_ref[LANES:, :], preferred_element_type=jnp.float32)
        right = state_ref[:padded, :].astype(jnp.float32) + lap * pull
        right = right.astype(jnp.bfloat16)
        edge = jnp.dot(spread_ref[...], right[LANES:], preferred_element_type=jnp.float32)
        start = pl.multiple_of(FRONT + step * TILE, 256)
        xm[pl.ds(start, TILE), :] = jnp.transpose(right[:LANES].astype(jnp.float32))
        xe[pl.ds(start, TILE), :] = jnp.transpose(edge)

    @pl.when(step == streams)
    def _():
        def regroup(s, carry):
            order = jnp.maximum(orders_ref[s], 0)
            base = FRONT + s * slot_width
            for p in range(2):
                for x, low, up in ((xm, lm, um), (xe, le, ue)):
                    up[pl.ds(2 * s + p, half, stride=UP), :] = x[
                        pl.ds(base + 2 * (half + 1) + p, half, stride=2), :
                    ]
                    low[pl.ds(2 * s + p, half, stride=LOW), :] = x[
                        pl.ds(base - 2 * order + p, half, stride=2), :
                    ]
                    up[pl.ds(2 * (slot_count + s) + p, half, stride=UP), :] = x[
                        pl.ds(base + 2 * (half - order) + p, half, stride=2), :
                    ]

                    @pl.when(orders_ref[s] >= 0)
                    def _(x=x, up=up, p=p):
                        third = UP * (half - 1 - order) + 4 * slot_count + p
                        up[pl.ds(third, 1), :] = x[
                            pl.ds(base + 2 * (truncation + 1 - order) + p, 1), :
                        ]

            return carry

        lax.fori_loop(0, slot_count, regroup, 0)

    @pl.when(step >= streams)
    def _():
        row = lax.broadcasted_iota(jnp.int32, (16, LANES), 0)
        order_rows = jnp.full((16, LANES), BIG, jnp.int32)
        for s in range(slot_count):
            order_rows = jnp.where(row // 2 == s, jnp.maximum(orders_ref[s], 0), order_rows)
        mask = edge_masks(slot_count, levels - LANES, (ROWS, LANES), 0)
        tail = lax.broadcasted_iota(jnp.int32, (8, LANES), 0) >= 6
        count = out_ref.shape[0] // pair_count
        first = (step - streams) * count

        def assemble(d, j):
            n = index_ref[first + d, j]
            start = UP * (half - 1 - n)
            low = LOW * n
            body = um[pl.ds(start, ROWS), :]
            edge = ue[pl.ds(start, ROWS), :]
            own = order_rows <= n
            top = jnp.where(own, lm[pl.ds(low, 16), :], body[:16])
            top_edge = jnp.where(own, le[pl.ds(low, 16), :], edge[:16])
            folded = parity_fold(
                [
                    jnp.where(mask[:8], top_edge[:8], 0.0),
                    jnp.where(mask[8:16], top_edge[8:], 0.0),
                    jnp.where(mask[16:], edge[16:], 0.0),
                ],
                0,
            )
            block = jnp.concatenate([top, jnp.where(tail, folded, body[16:])], axis=0)
            out_ref[d * pair_count + j] = block.astype(jnp.bfloat16)

        def assemble_all(d, carry):
            for j in range(pair_count):
                assemble(d, j)
            return carry

        lax.fori_loop(0, count, assemble_all, 0, unroll=2)


def solve_kernel(sizes, lows_ref, index_ref, blocks_ref, weights_ref, out_ref):
    levels, slot_count = sizes
    count, pair_count = blocks_ref.shape[0], blocks_ref.shape[1]
    shape = (count, ROWS, LANES)
    mask = edge_masks(slot_count, levels - LANES, shape, 1)
    row = lax.broadcasted_iota(jnp.int32, shape, 1)
    slot = lax.broadcasted_iota(jnp.int32, (16, LANES), 0) // 2
    orders = []
    for k in range(count):
        lines = jnp.full((16, LANES), BIG, jnp.int32)
        for s in range(slot_count):
            order = index_ref[pl.program_id(0) * count + k, pair_count + s]
            lines = jnp.where(slot == s, order, lines)
        orders.append(lines)
    orders = jnp.stack(orders)
    for j in range(pair_count):
        body = blocks_ref[:, j].astype(jnp.float32)
        edge = jnp.where(row % 2 == 0, body[:, ROWS - 2 : ROWS - 1], body[:, ROWS - 1 :])
        edge = jnp.where(mask, edge, 0.0)
        lines = jnp.concatenate([body, edge], axis=-1)
        top = lines[:, :16].reshape(count * 16, 2 * LANES).astype(jnp.bfloat16)
        lines = lines.reshape(count * ROWS, 2 * LANES).astype(jnp.bfloat16)
        upper = jnp.dot(lines, weights_ref[j, 1], preferred_element_type=jnp.float32)
        upper = upper.reshape(count, ROWS, 2 * LANES)
        lower = jnp.dot(top, weights_ref[j, 0], preferred_element_type=jnp.float32)
        lower = lower.reshape(count, 16, 2 * LANES)
        own = orders <= lows_ref[j]
        main = jnp.where(own, lower[..., :LANES], upper[:, :16, :LANES])
        edge = jnp.where(own, lower[..., LANES:], upper[:, :16, LANES:])
        edge = jnp.where(mask[:, :16], edge, 0.0)
        rest = jnp.where(mask[:, 16:], upper[:, 16:, LANES:], 0.0)
        folded = parity_fold([edge[:, :8], edge[:, 8:], rest], 1)
        rest = jnp.where(row[:, 16:] >= ROWS - 2, folded, upper[:, 16:, :LANES])
        out_ref[:, j] = jnp.concatenate([main, rest], axis=1).astype(jnp.bfloat16)


def final_kernel(
    sizes,
    index_ref,
    orders_ref,
    blocks_ref,
    state_ref,
    last_ref,
    weights_ref,
    out_ref,
    xm,
    xe,
    lm,
    le,
    um,
    ue,
):
    levels, slot_count, slot_width, truncation, pair_count, streams = sizes
    half = (truncation + 1) // 2
    step = pl.program_id(0)

    @pl.when(step < streams)
    def _():
        mask = edge_masks(slot_count, levels - LANES, (ROWS, LANES), 0)
        even = lax.broadcasted_iota(jnp.int32, (ROWS, LANES), 0) % 2 == 0
        count = blocks_ref.shape[0] // pair_count
        first = step * count

        def unfold(d, carry):
            for j in range(pair_count):
                n = index_ref[first + d, j]
                body = blocks_ref[d * pair_count + j].astype(jnp.float32)
                edge = jnp.where(even, body[ROWS - 2 : ROWS - 1], body[ROWS - 1 :])
                edge = jnp.where(mask, edge, 0.0)
                start = UP * (half - 1 - n)
                low = LOW * n
                um[pl.ds(start, ROWS), :] = body
                ue[pl.ds(start, ROWS), :] = edge
                lm[pl.ds(low, 16), :] = body[:16]
                le[pl.ds(low, 16), :] = edge[:16]
            return carry

        lax.fori_loop(0, count, unfold, 0, unroll=2)

    @pl.when(step == streams)
    def _():
        def regroup(k, carry):
            s = slot_count - 1 - k
            order = jnp.maximum(orders_ref[s], 0)
            base = FRONT + s * slot_width
            for p in range(2):
                for x, low, up in ((xm, lm, um), (xe, le, ue)):
                    x[pl.ds(base + 2 * (half + 1) + p, half, stride=2), :] = up[
                        pl.ds(2 * s + p, half, stride=UP), :
                    ]
                    x[pl.ds(base - 2 * order + p, half, stride=2), :] = low[
                        pl.ds(2 * s + p, half, stride=LOW), :
                    ]
                    x[pl.ds(base + 2 * (half - order) + p, half, stride=2), :] = up[
                        pl.ds(2 * (slot_count + s) + p, half, stride=UP), :
                    ]
                third = UP * (half - 1 - order) + 4 * slot_count + p
                place = base + 2 * (truncation + 1 - order) + p
                xm[pl.ds(place, 1), :] = um[pl.ds(third, 1), :]
                xe[pl.ds(place, 1), :] = ue[pl.ds(third, 1), :]
            return carry

        lax.fori_loop(0, slot_count, regroup, 0)

    @pl.when(step >= streams)
    def _():
        tile = step - streams
        start = pl.multiple_of(FRONT + tile * TILE, 256)
        lines = jnp.concatenate([xm[pl.ds(start, TILE), :], xe[pl.ds(start, TILE), :]], axis=1)
        moved = lax.dot_general(
            weights_ref[...],
            lines.astype(jnp.bfloat16),
            (((1,), (1,)), ((), ())),
            preferred_element_type=jnp.float32,
        )
        columns = tile * TILE + lax.broadcasted_iota(jnp.int32, (1, TILE), 1)
        order, _ = slot_lines(columns, orders_ref, slot_count, slot_width)
        moved = jnp.where(order >= 0, moved, 0.0)
        head = state_ref.shape[0]
        split = 2 * head
        held = lax.broadcasted_iota(jnp.int32, (head, 1), 0) >= levels - head
        held = held & (order >= 0)
        kept = jnp.where(held, state_ref[...].astype(jnp.float32), 0.0)
        out_ref[:head, :] = moved[:head].astype(jnp.bfloat16)
        out_ref[head:split, :] = (kept + moved[head:split]).astype(jnp.bfloat16)
        rest = out_ref.shape[0] - split
        kept = jnp.where(order >= 0, last_ref[:rest, :].astype(jnp.float32), 0.0)
        out_ref[split:, :] = (kept + moved[split:]).astype(jnp.bfloat16)


def level_of_lane(levels, slot_count):
    edge = levels - LANES
    table = np.zeros((2 * LANES, levels), np.float32)
    table[np.arange(LANES), np.arange(LANES)] = 1.0
    folded = np.arange(edge * (2 * slot_count + 1))
    table[LANES + folded, LANES + folded % edge] = 1.0
    return table


def shards(
    state,
    held_orders,
    pair_lows,
    inverses,
    height_operator,
    pressure_column,
    thermal_response_matrix,
    mass_row,
):
    levels = height_operator.shape[0]
    pair_count = pair_lows.shape[0]
    slot_count = held_orders.shape[0]
    devices = lax.axis_size(GRP_WAVE)
    half = pair_count * devices
    truncation = 2 * half - 1
    slot_width = 2 * (truncation + 2)
    width = slot_count * slot_width
    rows = state.shape[0]
    steps = -(-width // TILE)
    bf16, f32 = jnp.bfloat16, jnp.float32
    vmem = pl.BlockSpec(memory_space=pltpu.VMEM)
    smem = pl.BlockSpec(memory_space=pltpu.SMEM)

    def params(mib):
        return pltpu.CompilerParams(vmem_limit_bytes=mib * 1024 * 1024)

    scratch = [
        pltpu.VMEM((FRONT + steps * TILE, LANES), f32),
        pltpu.VMEM((FRONT + steps * TILE, LANES), f32),
        pltpu.VMEM((LOW * half, LANES), f32),
        pltpu.VMEM((LOW * half, LANES), f32),
        pltpu.VMEM((UP * half, LANES), f32),
        pltpu.VMEM((UP * half, LANES), f32),
    ]

    own = jnp.concatenate([pair_lows, held_orders])
    own = jnp.pad(own, (0, LANES - own.shape[0]))
    index = lax.all_to_all(
        jnp.broadcast_to(own[None, None], (devices, 1, LANES)), GRP_WAVE, 0, 0, tiled=True
    ).reshape(devices, LANES)

    table = level_of_lane(levels, slot_count)
    padded = -(-levels // 16) * 16
    spread = np.zeros((LANES, padded - LANES), np.float32)
    spread[:, : levels - LANES] = table[LANES:, LANES:]
    place = np.zeros((levels, rows - LANES), np.float32)
    place[:, levels - LANES : 2 * levels - LANES] = np.eye(levels)
    table, spread, place = (jnp.asarray(x, bf16) for x in (table, spread, place))
    eye = jnp.asarray(np.eye(256), bf16)

    message = pl.pallas_call(
        functools.partial(rhs_kernel, (levels, slot_count, slot_width, truncation, pair_count, steps)),
        grid=(2 * steps,),
        in_specs=[
            smem,
            smem,
            pl.BlockSpec((rows, TILE), lambda i: (0, jnp.minimum(i, steps - 1))),
            vmem,
            vmem,
            vmem,
            vmem,
            vmem,
        ],
        out_specs=pl.BlockSpec(
            (half // steps, ROWS, LANES), lambda i: (jnp.maximum(i - steps, 0), 0, 0)
        ),
        out_shape=jax.ShapeDtypeStruct((half, ROWS, LANES), bf16),
        scratch_shapes=[pltpu.VMEM((padded, rows - LANES), bf16)] + scratch,
        compiler_params=params(56),
        name="right_side",
    )(index, held_orders, state, height_operator, pressure_column, place, spread, eye)

    arrived = lax.all_to_all(
        message.reshape(devices, pair_count * ROWS, LANES), GRP_WAVE, 0, 0, tiled=True
    ).reshape(devices, pair_count, ROWS, LANES)

    weights = jnp.einsum("al,jtkl->jtak", table, inverses, preferred_element_type=f32)
    weights = jnp.einsum("jtak,bk->jtab", weights.astype(bf16), table, preferred_element_type=f32)
    weights = weights.astype(bf16)
    chunk = 16
    solved = pl.pallas_call(
        functools.partial(solve_kernel, (levels, slot_count)),
        grid=(devices // chunk,),
        in_specs=[
            smem,
            smem,
            pl.BlockSpec((chunk, pair_count, ROWS, LANES), lambda i: (i, 0, 0, 0)),
            vmem,
        ],
        out_specs=pl.BlockSpec((chunk, pair_count, ROWS, LANES), lambda i: (i, 0, 0, 0)),
        out_shape=jax.ShapeDtypeStruct((devices, pair_count, ROWS, LANES), bf16),
        compiler_params=params(52),
        name="solve",
    )(pair_lows, index, arrived, weights)

    returned = lax.all_to_all(
        solved.reshape(devices, pair_count * ROWS, LANES), GRP_WAVE, 0, 0, tiled=True
    ).reshape(half, ROWS, LANES)

    head = levels // 8 * 8
    response = jnp.concatenate(
        [jnp.eye(levels, dtype=bf16), -thermal_response_matrix, -mass_row[None, :]], axis=0
    )
    response = jnp.dot(response, table.T, preferred_element_type=f32).astype(bf16)
    return pl.pallas_call(
        functools.partial(final_kernel, (levels, slot_count, slot_width, truncation, pair_count, steps)),
        grid=(2 * steps,),
        in_specs=[
            smem,
            smem,
            pl.BlockSpec((half // steps, ROWS, LANES), lambda i: (jnp.minimum(i, steps - 1), 0, 0)),
            pl.BlockSpec((head, TILE), lambda i: (1, jnp.maximum(i - steps, 0))),
            pl.BlockSpec((8, TILE), lambda i: (2 * head // 8, jnp.maximum(i - steps, 0))),
            vmem,
        ],
        out_specs=pl.BlockSpec((rows, TILE), lambda i: (0, jnp.maximum(i - steps, 0))),
        out_shape=jax.ShapeDtypeStruct((rows, width), bf16),
        scratch_shapes=scratch,
        compiler_params=params(48),
        name="final",
    )(index, held_orders, returned, state, state, response)


def solution(mesh):
    torus = Mesh(
        mesh.devices.reshape(mesh.shape["grp"], 4, 4, 2), ("grp", "wave_0", "wave_1", "wave_2")
    )
    placed = (
        P(None, GRP_WAVE),
        P(GRP_WAVE),
        P(GRP_WAVE),
        P(GRP_WAVE, None, None, None),
        P(),
        P(),
        P(),
        P(),
    )
    return jax.shard_map(
        shards, mesh=torus, in_specs=placed, out_specs=P(None, GRP_WAVE), check_vma=False
    )
```

```python
import functools

import jax
import jax.numpy as jnp
import numpy as np
from jax import lax
from jax.experimental import pallas as pl
from jax.experimental.pallas import tpu as pltpu
from jax.sharding import Mesh
from jax.sharding import PartitionSpec as P

GRP_WAVE = ("grp", "wave_0", "wave_1", "wave_2")

LANES = 128
ROWS = 24
FRONT = 768
WORDS = 8
TILE = 3968
BIG = 1 << 20
LOW = 17
UP = 25


def edge_masks(slot_count, edge, shape, row_dim):
    rows = lax.broadcasted_iota(jnp.int32, shape, row_dim)
    lanes = lax.broadcasted_iota(jnp.int32, shape, len(shape) - 1)
    group = rows // 2
    return (lanes >= edge * group) & (lanes < edge * (group + 1)) & (rows < 4 * slot_count + 2)


def parity_fold(parts, axis):
    total = parts[0]
    for part in parts[1:]:
        total = total + part
    total = total + pltpu.roll(total, 2, axis)
    return total + pltpu.roll(total, 4, axis)


def slot_lines(columns, orders_ref, slot_count, slot_width):
    order = jnp.full(columns.shape, -1, jnp.int32)
    place = columns
    for s in range(slot_count):
        inside = (columns >= s * slot_width) & (columns < (s + 1) * slot_width)
        order = jnp.where(inside, orders_ref[s], order)
        place = jnp.where(inside, columns - s * slot_width, place)
    return order, place // 2


def rhs_kernel(
    sizes,
    index_ref,
    orders_ref,
    state_ref,
    height_ref,
    pressure_ref,
    place_ref,
    spread_ref,
    eye_ref,
    out_ref,
    near,
    index_sem,
    drive,
    xm,
    xe,
    lm,
    le,
    um,
    ue,
):
    levels, slot_count, slot_width, truncation, pair_count, streams = sizes
    half = (truncation + 1) // 2
    step = pl.program_id(0)
    fetch = pltpu.make_async_copy(index_ref, near, index_sem)

    @pl.when(step == 0)
    def _():
        fetch.start()
        moved = jnp.dot(height_ref[...], place_ref[...], preferred_element_type=jnp.float32)
        row = jnp.broadcast_to(pressure_ref[...].reshape(1, levels), (LANES, levels))
        column = lax.dot_general(
            eye_ref[:levels, :levels],
            row,
            (((1,), (1,)), ((), ())),
            preferred_element_type=jnp.float32,
        )
        last = lax.broadcasted_iota(jnp.int32, moved.shape, 1) == moved.shape[1] - 1
        moved = jnp.where(last, column[:, :1], moved).astype(jnp.bfloat16)
        drive[...] = jnp.zeros_like(drive)
        drive[:levels, :] = moved

    @pl.when(step < streams)
    def _():
        columns = step * TILE + lax.broadcasted_iota(jnp.int32, (1, TILE), 1)
        order, coeff = slot_lines(columns, orders_ref, slot_count, slot_width)
        degree = jnp.where(coeff <= truncation - order, order + coeff, coeff - 1)
        lap = (degree * (degree + 1)).astype(jnp.float32) / float(truncation * (truncation + 1))
        padded = drive.shape[0]
        pull = jnp.dot(drive[...], state_ref[LANES:, :], preferred_element_type=jnp.float32)
        right = state_ref[:padded, :].astype(jnp.float32) + lap * pull
        right = right.astype(jnp.bfloat16)
        edge = jnp.dot(spread_ref[...], right[LANES:], preferred_element_type=jnp.float32)
        start = pl.multiple_of(FRONT + step * TILE, 256)
        xm[pl.ds(start, TILE), :] = jnp.transpose(right[:LANES].astype(jnp.float32))
        xe[pl.ds(start, TILE), :] = jnp.transpose(edge)

    @pl.when(step == streams)
    def _():
        fetch.wait()

        def regroup(s, carry):
            order = jnp.maximum(orders_ref[s], 0)
            base = FRONT + s * slot_width
            for p in range(2):
                for x, low, up in ((xm, lm, um), (xe, le, ue)):
                    up[pl.ds(2 * s + p, half, stride=UP), :] = x[
                        pl.ds(base + 2 * (half + 1) + p, half, stride=2), :
                    ]
                    low[pl.ds(2 * s + p, half, stride=LOW), :] = x[
                        pl.ds(base - 2 * order + p, half, stride=2), :
                    ]
                    up[pl.ds(2 * (slot_count + s) + p, half, stride=UP), :] = x[
                        pl.ds(base + 2 * (half - order) + p, half, stride=2), :
                    ]

                    @pl.when(orders_ref[s] >= 0)
                    def _(x=x, up=up, p=p):
                        third = UP * (half - 1 - order) + 4 * slot_count + p
                        up[pl.ds(third, 1), :] = x[
                            pl.ds(base + 2 * (truncation + 1 - order) + p, 1), :
                        ]

            return carry

        lax.fori_loop(0, slot_count, regroup, 0)

    @pl.when(step >= streams)
    def _():
        row = lax.broadcasted_iota(jnp.int32, (16, LANES), 0)
        order_rows = jnp.full((16, LANES), BIG, jnp.int32)
        for s in range(slot_count):
            order_rows = jnp.where(row // 2 == s, jnp.maximum(orders_ref[s], 0), order_rows)
        mask = edge_masks(slot_count, levels - LANES, (ROWS, LANES), 0)
        tail = lax.broadcasted_iota(jnp.int32, (8, LANES), 0) >= 6
        count = out_ref.shape[0] // pair_count
        first = (step - streams) * count

        def assemble(d, j):
            n = near[first + d, j]
            start = UP * (half - 1 - n)
            low = LOW * n
            body = um[pl.ds(start, ROWS), :]
            edge = ue[pl.ds(start, ROWS), :]
            own = order_rows <= n
            top = jnp.where(own, lm[pl.ds(low, 16), :], body[:16])
            top_edge = jnp.where(own, le[pl.ds(low, 16), :], edge[:16])
            folded = parity_fold(
                [
                    jnp.where(mask[:8], top_edge[:8], 0.0),
                    jnp.where(mask[8:16], top_edge[8:], 0.0),
                    jnp.where(mask[16:], edge[16:], 0.0),
                ],
                0,
            )
            block = jnp.concatenate([top, jnp.where(tail, folded, body[16:])], axis=0)
            out_ref[d * pair_count + j] = block.astype(jnp.bfloat16)

        def assemble_all(d, carry):
            for j in range(pair_count):
                assemble(d, j)
            return carry

        lax.fori_loop(0, count, assemble_all, 0, unroll=2)


def solve_kernel(sizes, lows_ref, index_ref, blocks_ref, weights_ref, out_ref):
    levels, slot_count = sizes
    count, pair_count = blocks_ref.shape[0], blocks_ref.shape[1]
    shape = (count, ROWS, LANES)
    mask = edge_masks(slot_count, levels - LANES, shape, 1)
    row = lax.broadcasted_iota(jnp.int32, shape, 1)
    slot = lax.broadcasted_iota(jnp.int32, (16, LANES), 0) // 2
    orders = []
    for k in range(count):
        lines = jnp.full((16, LANES), BIG, jnp.int32)
        for s in range(slot_count):
            order = index_ref[(pl.program_id(0) * count + k) * WORDS + pair_count + s]
            lines = jnp.where(slot == s, order, lines)
        orders.append(lines)
    orders = jnp.stack(orders)
    for j in range(pair_count):
        body = blocks_ref[:, j].astype(jnp.float32)
        edge = jnp.where(row % 2 == 0, body[:, ROWS - 2 : ROWS - 1], body[:, ROWS - 1 :])
        edge = jnp.where(mask, edge, 0.0)
        lines = jnp.concatenate([body, edge], axis=-1)
        top = lines[:, :16].reshape(count * 16, 2 * LANES).astype(jnp.bfloat16)
        lines = lines.reshape(count * ROWS, 2 * LANES).astype(jnp.bfloat16)
        upper = jnp.dot(lines, weights_ref[j, 1], preferred_element_type=jnp.float32)
        upper = upper.reshape(count, ROWS, 2 * LANES)
        lower = jnp.dot(top, weights_ref[j, 0], preferred_element_type=jnp.float32)
        lower = lower.reshape(count, 16, 2 * LANES)
        own = orders <= lows_ref[j]
        main = jnp.where(own, lower[..., :LANES], upper[:, :16, :LANES])
        edge = jnp.where(own, lower[..., LANES:], upper[:, :16, LANES:])
        edge = jnp.where(mask[:, :16], edge, 0.0)
        rest = jnp.where(mask[:, 16:], upper[:, 16:, LANES:], 0.0)
        folded = parity_fold([edge[:, :8], edge[:, 8:], rest], 1)
        rest = jnp.where(row[:, 16:] >= ROWS - 2, folded, upper[:, 16:, :LANES])
        out_ref[:, j] = jnp.concatenate([main, rest], axis=1).astype(jnp.bfloat16)


def final_kernel(
    sizes,
    index_ref,
    orders_ref,
    blocks_ref,
    state_ref,
    last_ref,
    weights_ref,
    out_ref,
    xm,
    xe,
    lm,
    le,
    um,
    ue,
):
    levels, slot_count, slot_width, truncation, pair_count, streams = sizes
    half = (truncation + 1) // 2
    step = pl.program_id(0)

    @pl.when(step < streams)
    def _():
        mask = edge_masks(slot_count, levels - LANES, (ROWS, LANES), 0)
        even = lax.broadcasted_iota(jnp.int32, (ROWS, LANES), 0) % 2 == 0
        count = blocks_ref.shape[0] // pair_count
        first = step * count

        def unfold(d, carry):
            for j in range(pair_count):
                n = index_ref[(first + d) * WORDS + j]
                body = blocks_ref[d * pair_count + j].astype(jnp.float32)
                edge = jnp.where(even, body[ROWS - 2 : ROWS - 1], body[ROWS - 1 :])
                edge = jnp.where(mask, edge, 0.0)
                start = UP * (half - 1 - n)
                low = LOW * n
                um[pl.ds(start, ROWS), :] = body
                ue[pl.ds(start, ROWS), :] = edge
                lm[pl.ds(low, 16), :] = body[:16]
                le[pl.ds(low, 16), :] = edge[:16]
            return carry

        lax.fori_loop(0, count, unfold, 0, unroll=2)

    @pl.when(step == streams)
    def _():
        def regroup(k, carry):
            s = slot_count - 1 - k
            order = jnp.maximum(orders_ref[s], 0)
            base = FRONT + s * slot_width
            for p in range(2):
                for x, low, up in ((xm, lm, um), (xe, le, ue)):
                    x[pl.ds(base + 2 * (half + 1) + p, half, stride=2), :] = up[
                        pl.ds(2 * s + p, half, stride=UP), :
                    ]
                    x[pl.ds(base - 2 * order + p, half, stride=2), :] = low[
                        pl.ds(2 * s + p, half, stride=LOW), :
                    ]
                    x[pl.ds(base + 2 * (half - order) + p, half, stride=2), :] = up[
                        pl.ds(2 * (slot_count + s) + p, half, stride=UP), :
                    ]
                third = UP * (half - 1 - order) + 4 * slot_count + p
                place = base + 2 * (truncation + 1 - order) + p
                xm[pl.ds(place, 1), :] = um[pl.ds(third, 1), :]
                xe[pl.ds(place, 1), :] = ue[pl.ds(third, 1), :]
            return carry

        lax.fori_loop(0, slot_count, regroup, 0)

    @pl.when(step >= streams)
    def _():
        tile = step - streams
        start = pl.multiple_of(FRONT + tile * TILE, 256)
        lines = jnp.concatenate([xm[pl.ds(start, TILE), :], xe[pl.ds(start, TILE), :]], axis=1)
        moved = lax.dot_general(
            weights_ref[...],
            lines.astype(jnp.bfloat16),
            (((1,), (1,)), ((), ())),
            preferred_element_type=jnp.float32,
        )
        columns = tile * TILE + lax.broadcasted_iota(jnp.int32, (1, TILE), 1)
        order, _ = slot_lines(columns, orders_ref, slot_count, slot_width)
        moved = jnp.where(order >= 0, moved, 0.0)
        head = state_ref.shape[0]
        split = 2 * head
        held = lax.broadcasted_iota(jnp.int32, (head, 1), 0) >= levels - head
        held = held & (order >= 0)
        kept = jnp.where(held, state_ref[...].astype(jnp.float32), 0.0)
        out_ref[:head, :] = moved[:head].astype(jnp.bfloat16)
        out_ref[head:split, :] = (kept + moved[head:split]).astype(jnp.bfloat16)
        rest = out_ref.shape[0] - split
        kept = jnp.where(order >= 0, last_ref[:rest, :].astype(jnp.float32), 0.0)
        out_ref[split:, :] = (kept + moved[split:]).astype(jnp.bfloat16)


def level_of_lane(levels, slot_count):
    edge = levels - LANES
    table = np.zeros((2 * LANES, levels), np.float32)
    table[np.arange(LANES), np.arange(LANES)] = 1.0
    folded = np.arange(edge * (2 * slot_count + 1))
    table[LANES + folded, LANES + folded % edge] = 1.0
    return table


def shards(
    state,
    held_orders,
    pair_lows,
    inverses,
    height_operator,
    pressure_column,
    thermal_response_matrix,
    mass_row,
):
    levels = height_operator.shape[0]
    pair_count = pair_lows.shape[0]
    slot_count = held_orders.shape[0]
    devices = lax.axis_size(GRP_WAVE)
    half = pair_count * devices
    truncation = 2 * half - 1
    slot_width = 2 * (truncation + 2)
    width = slot_count * slot_width
    rows = state.shape[0]
    steps = -(-width // TILE)
    bf16, f32 = jnp.bfloat16, jnp.float32
    vmem = pl.BlockSpec(memory_space=pltpu.VMEM)
    smem = pl.BlockSpec(memory_space=pltpu.SMEM)

    def params(mib):
        return pltpu.CompilerParams(vmem_limit_bytes=mib * 1024 * 1024)

    scratch = [
        pltpu.VMEM((FRONT + steps * TILE, LANES), f32),
        pltpu.VMEM((FRONT + steps * TILE, LANES), f32),
        pltpu.VMEM((LOW * half, LANES), f32),
        pltpu.VMEM((LOW * half, LANES), f32),
        pltpu.VMEM((UP * half, LANES), f32),
        pltpu.VMEM((UP * half, LANES), f32),
    ]

    own = jnp.concatenate([pair_lows, held_orders])
    own = jnp.pad(own, (0, LANES - own.shape[0]))
    index = lax.all_to_all(
        jnp.broadcast_to(own[None, None], (devices, 1, LANES)), GRP_WAVE, 0, 0, tiled=True
    ).reshape(devices, LANES)

    table = level_of_lane(levels, slot_count)
    padded = -(-levels // 16) * 16
    spread = np.zeros((LANES, padded - LANES), np.float32)
    spread[:, : levels - LANES] = table[LANES:, LANES:]
    place = np.zeros((levels, rows - LANES), np.float32)
    place[:, levels - LANES : 2 * levels - LANES] = np.eye(levels)
    table, spread, place = (jnp.asarray(x, bf16) for x in (table, spread, place))
    eye = jnp.asarray(np.eye(256), bf16)

    message = pl.pallas_call(
        functools.partial(rhs_kernel, (levels, slot_count, slot_width, truncation, pair_count, steps)),
        grid=(2 * steps,),
        in_specs=[
            pl.BlockSpec(memory_space=pl.ANY),
            smem,
            pl.BlockSpec((rows, TILE), lambda i: (0, jnp.minimum(i, steps - 1))),
            vmem,
            vmem,
            vmem,
            vmem,
            vmem,
        ],
        out_specs=pl.BlockSpec(
            (half // steps, ROWS, LANES), lambda i: (jnp.maximum(i - steps, 0), 0, 0)
        ),
        out_shape=jax.ShapeDtypeStruct((half, ROWS, LANES), bf16),
        scratch_shapes=[
            pltpu.SMEM((devices, LANES), jnp.int32),
            pltpu.SemaphoreType.DMA,
            pltpu.VMEM((padded, rows - LANES), bf16),
        ]
        + scratch,
        compiler_params=params(56),
        name="right_side",
    )(index, held_orders, state, height_operator, pressure_column, place, spread, eye)

    arrived = lax.all_to_all(
        message.reshape(devices, pair_count * ROWS, LANES), GRP_WAVE, 0, 0, tiled=True
    ).reshape(devices, pair_count, ROWS, LANES)

    weights = jnp.einsum("al,jtkl->jtak", table, inverses, preferred_element_type=f32)
    weights = jnp.einsum("jtak,bk->jtab", weights.astype(bf16), table, preferred_element_type=f32)
    weights = weights.astype(bf16)
    words = index[:, :WORDS].reshape(-1)
    chunk = 64
    solved = pl.pallas_call(
        functools.partial(solve_kernel, (levels, slot_count)),
        grid=(devices // chunk,),
        in_specs=[
            smem,
            smem,
            pl.BlockSpec((chunk, pair_count, ROWS, LANES), lambda i: (i, 0, 0, 0)),
            vmem,
        ],
        out_specs=pl.BlockSpec((chunk, pair_count, ROWS, LANES), lambda i: (i, 0, 0, 0)),
        out_shape=jax.ShapeDtypeStruct((devices, pair_count, ROWS, LANES), bf16),
        compiler_params=params(52),
        name="solve",
    )(pair_lows, words, arrived, weights)

    returned = lax.all_to_all(
        solved.reshape(devices, pair_count * ROWS, LANES), GRP_WAVE, 0, 0, tiled=True
    ).reshape(half, ROWS, LANES)

    head = levels // 8 * 8
    response = jnp.concatenate(
        [jnp.eye(levels, dtype=bf16), -thermal_response_matrix, -mass_row[None, :]], axis=0
    )
    response = jnp.dot(response, table.T, preferred_element_type=f32).astype(bf16)
    return pl.pallas_call(
        functools.partial(final_kernel, (levels, slot_count, slot_width, truncation, pair_count, steps)),
        grid=(2 * steps,),
        in_specs=[
            smem,
            smem,
            pl.BlockSpec((half // steps, ROWS, LANES), lambda i: (jnp.minimum(i, steps - 1), 0, 0)),
            pl.BlockSpec((head, TILE), lambda i: (1, jnp.maximum(i - steps, 0))),
            pl.BlockSpec((8, TILE), lambda i: (2 * head // 8, jnp.maximum(i - steps, 0))),
            vmem,
        ],
        out_specs=pl.BlockSpec((rows, TILE), lambda i: (0, jnp.maximum(i - steps, 0))),
        out_shape=jax.ShapeDtypeStruct((rows, width), bf16),
        scratch_shapes=scratch,
        compiler_params=params(48),
        name="final",
    )(words, held_orders, returned, state, state, response)


def solution(mesh):
    torus = Mesh(
        mesh.devices.reshape(mesh.shape["grp"], 4, 4, 2), ("grp", "wave_0", "wave_1", "wave_2")
    )
    placed = (
        P(None, GRP_WAVE),
        P(GRP_WAVE),
        P(GRP_WAVE),
        P(GRP_WAVE, None, None, None),
        P(),
        P(),
        P(),
        P(),
    )
    return jax.shard_map(
        shards, mesh=torus, in_specs=placed, out_specs=P(None, GRP_WAVE), check_vma=False
    )
```

```python
import functools

import jax
import jax.numpy as jnp
import numpy as np
from jax import lax
from jax.experimental import pallas as pl
from jax.experimental.pallas import tpu as pltpu
from jax.sharding import Mesh
from jax.sharding import PartitionSpec as P

GRP_WAVE = ("grp", "wave_0", "wave_1", "wave_2")

LANES = 128
ROWS = 24
FRONT = 768
WORDS = 8
TILE = 3840
PARTS = 4
BIG = 1 << 20
LOW = 17
UP = 25


def edge_masks(slot_count, edge, shape, row_dim):
    rows = lax.broadcasted_iota(jnp.int32, shape, row_dim)
    lanes = lax.broadcasted_iota(jnp.int32, shape, len(shape) - 1)
    group = rows // 2
    return (lanes >= edge * group) & (lanes < edge * (group + 1)) & (rows < 4 * slot_count + 2)


def parity_fold(parts, axis):
    total = parts[0]
    for part in parts[1:]:
        total = total + part
    total = total + pltpu.roll(total, 2, axis)
    return total + pltpu.roll(total, 4, axis)


def slot_lines(columns, orders_ref, slot_count, slot_width):
    order = jnp.full(columns.shape, -1, jnp.int32)
    place = columns
    for s in range(slot_count):
        inside = (columns >= s * slot_width) & (columns < (s + 1) * slot_width)
        order = jnp.where(inside, orders_ref[s], order)
        place = jnp.where(inside, columns - s * slot_width, place)
    return order, place // 2


def column_parts(width):
    starts = list(range(0, width - TILE // 2, TILE))
    return [(a, b - a) for a, b in zip(starts, starts[1:] + [width])]


def state_copies(state_ref, first, body, tail, sems):
    copies = []
    parts = column_parts(state_ref.shape[1])
    for k, (start, size) in enumerate(parts):
        source = state_ref.at[pl.ds(first, body.shape[0]), pl.ds(start, size)]
        target = tail if k == len(parts) - 1 else body.at[:, pl.ds(start, size)]
        copies.append(pltpu.make_async_copy(source, target, sems.at[k]))
    return copies


def rhs_kernel(
    sizes,
    index_ref,
    orders_ref,
    state_ref,
    height_ref,
    pressure_ref,
    out_ref,
    near,
    index_sem,
    height,
    height_sem,
    drive,
    body,
    tail,
    state_sems,
    stage,
    out_sems,
    xm,
    xe,
    lm,
    le,
    um,
    ue,
):
    levels, slot_count, slot_width, truncation, pair_count = sizes
    half = (truncation + 1) // 2
    parts = column_parts(state_ref.shape[1])
    bring = pltpu.make_async_copy(height_ref, height, height_sem)
    bring.start()
    copies = state_copies(state_ref, 0, body, tail, state_sems)
    for copy in copies:
        copy.start()
    fetch = pltpu.make_async_copy(index_ref, near, index_sem)
    fetch.start()

    edge_count = levels - LANES
    lane = lax.broadcasted_iota(jnp.int32, (LANES, drive.shape[0] - LANES), 0)
    group = jnp.zeros_like(lane)
    for g in range(1, 2 * slot_count + 2):
        group = group + jnp.where(lane >= edge_count * g, 1, 0)
    wanted = lax.broadcasted_iota(jnp.int32, lane.shape, 1) == lane - edge_count * group
    spread = jnp.where(wanted & (group <= 2 * slot_count), 1.0, 0.0).astype(jnp.bfloat16)
    column = jnp.broadcast_to(pressure_ref[...].reshape(1, levels).astype(jnp.float32), (8, levels))
    column = jnp.transpose(column)[:, :1]
    drive[...] = jnp.zeros_like(drive)
    last = drive.shape[1] - 1
    drive[:levels, last:] = column.astype(jnp.bfloat16)
    bring.wait()
    drive[:levels, last - levels : last] = height[...]
    padded = drive.shape[0]

    for k, (start, size) in enumerate(parts):
        copies[k].wait()
        if k == len(parts) - 1:
            upper, lower = tail[:padded, :], tail[LANES:, :]
        else:
            upper = body[:padded, start : start + size]
            lower = body[LANES:, start : start + size]
        columns = start + lax.broadcasted_iota(jnp.int32, (1, size), 1)
        order, coeff = slot_lines(columns, orders_ref, slot_count, slot_width)
        degree = jnp.where(coeff <= truncation - order, order + coeff, coeff - 1)
        lap = (degree * (degree + 1)).astype(jnp.float32) / float(truncation * (truncation + 1))
        pull = jnp.dot(drive[...], lower, preferred_element_type=jnp.float32)
        right = (upper.astype(jnp.float32) + lap * pull).astype(jnp.bfloat16)
        xm[pl.ds(FRONT + start, size), :] = jnp.transpose(right[:LANES].astype(jnp.float32))
        xe[pl.ds(FRONT + start, size), :] = lax.dot_general(
            jnp.transpose(right[LANES:].astype(jnp.float32)).astype(jnp.bfloat16),
            spread,
            (((1,), (1,)), ((), ())),
            preferred_element_type=jnp.float32,
        )

    def regroup(s, carry):
        order = jnp.maximum(orders_ref[s], 0)
        base = FRONT + s * slot_width
        for p in range(2):
            for x, low, up in ((xm, lm, um), (xe, le, ue)):
                up[pl.ds(2 * s + p, half, stride=UP), :] = x[
                    pl.ds(base + 2 * (half + 1) + p, half, stride=2), :
                ]
                low[pl.ds(2 * s + p, half, stride=LOW), :] = x[
                    pl.ds(base - 2 * order + p, half, stride=2), :
                ]
                up[pl.ds(2 * (slot_count + s) + p, half, stride=UP), :] = x[
                    pl.ds(base + 2 * (half - order) + p, half, stride=2), :
                ]

                @pl.when(orders_ref[s] >= 0)
                def _(x=x, up=up, p=p):
                    third = UP * (half - 1 - order) + 4 * slot_count + p
                    up[pl.ds(third, 1), :] = x[
                        pl.ds(base + 2 * (truncation + 1 - order) + p, 1), :
                    ]

        return carry

    lax.fori_loop(0, slot_count, regroup, 0)

    row = lax.broadcasted_iota(jnp.int32, (16, LANES), 0)
    order_rows = jnp.full((16, LANES), BIG, jnp.int32)
    for s in range(slot_count):
        order_rows = jnp.where(row // 2 == s, jnp.maximum(orders_ref[s], 0), order_rows)
    mask = edge_masks(slot_count, levels - LANES, (ROWS, LANES), 0)
    bottom = lax.broadcasted_iota(jnp.int32, (8, LANES), 0) >= 6

    def assemble(d, j):
        n = near[d, j]
        start = UP * (half - 1 - n)
        low = LOW * n
        lines = um[pl.ds(start, ROWS), :]
        edge = ue[pl.ds(start, ROWS), :]
        own = order_rows <= n
        top = jnp.where(own, lm[pl.ds(low, 16), :], lines[:16])
        top_edge = jnp.where(own, le[pl.ds(low, 16), :], edge[:16])
        folded = parity_fold(
            [
                jnp.where(mask[:8], top_edge[:8], 0.0),
                jnp.where(mask[8:16], top_edge[8:], 0.0),
                jnp.where(mask[16:], edge[16:], 0.0),
            ],
            0,
        )
        block = jnp.concatenate([top, jnp.where(bottom, folded, lines[16:])], axis=0)
        stage[d * pair_count + j] = block.astype(jnp.bfloat16)

    fetch.wait()
    count = half // pair_count // PARTS
    sends = []
    for k in range(PARTS):

        def assemble_all(d, carry):
            for j in range(pair_count):
                assemble(d, j)
            return carry

        lax.fori_loop(k * count, (k + 1) * count, assemble_all, 0, unroll=4)
        some = pl.ds(k * count * pair_count, count * pair_count)
        sends.append(pltpu.make_async_copy(stage.at[some], out_ref.at[some], out_sems.at[k]))
        sends[-1].start()
    for send in sends:
        send.wait()


def solve_kernel(
    sizes, lows_ref, index_ref, blocks_ref, weights_ref, out_ref, weights, sems, stage, out_sems
):
    levels, slot_count, chunk = sizes
    devices, pair_count = blocks_ref.shape[0], blocks_ref.shape[1]
    shape = (chunk, ROWS, LANES)
    mask = edge_masks(slot_count, levels - LANES, shape, 1)
    row = lax.broadcasted_iota(jnp.int32, shape, 1)
    slot = lax.broadcasted_iota(jnp.int32, (16, LANES), 0) // 2
    brings = []
    for j in range(pair_count):
        brings.append(pltpu.make_async_copy(weights_ref.at[j], weights.at[j], sems.at[j]))
        brings[-1].start()

    def solve_some(first):
        orders = []
        for k in range(chunk):
            lines = jnp.full((16, LANES), BIG, jnp.int32)
            for s in range(slot_count):
                order = index_ref[(first + k) * WORDS + pair_count + s]
                lines = jnp.where(slot == s, order, lines)
            orders.append(lines)
        orders = jnp.stack(orders)
        here = pl.ds(first, chunk)
        for j in range(pair_count):
            body = blocks_ref[here, j].astype(jnp.float32)
            edge = jnp.where(row % 2 == 0, body[:, ROWS - 2 : ROWS - 1], body[:, ROWS - 1 :])
            edge = jnp.where(mask, edge, 0.0)
            lines = jnp.concatenate([body, edge], axis=-1)
            top = lines[:, :16].reshape(chunk * 16, 2 * LANES).astype(jnp.bfloat16)
            lines = lines.reshape(chunk * ROWS, 2 * LANES).astype(jnp.bfloat16)
            pl.when(first == 0)(brings[j].wait)
            upper = jnp.dot(lines, weights[j, 1], preferred_element_type=jnp.float32)
            upper = upper.reshape(chunk, ROWS, 2 * LANES)
            lower = jnp.dot(top, weights[j, 0], preferred_element_type=jnp.float32)
            lower = lower.reshape(chunk, 16, 2 * LANES)
            own = orders <= lows_ref[j]
            main = jnp.where(own, lower[..., :LANES], upper[:, :16, :LANES])
            edge = jnp.where(own, lower[..., LANES:], upper[:, :16, LANES:])
            edge = jnp.where(mask[:, :16], edge, 0.0)
            rest = jnp.where(mask[:, 16:], upper[:, 16:, LANES:], 0.0)
            folded = parity_fold([edge[:, :8], edge[:, 8:], rest], 1)
            rest = jnp.where(row[:, 16:] >= ROWS - 2, folded, upper[:, 16:, :LANES])
            stage[here, j] = jnp.concatenate([main, rest], axis=1).astype(jnp.bfloat16)

    count = devices // PARTS
    sends = []
    for k in range(PARTS):

        def solve_all(c, carry):
            solve_some(k * count + c * chunk)
            return carry

        lax.fori_loop(0, count // chunk, solve_all, 0)
        some = pl.ds(k * count, count)
        sends.append(pltpu.make_async_copy(stage.at[some], out_ref.at[some], out_sems.at[k]))
        sends[-1].start()
    for send in sends:
        send.wait()


def final_kernel(
    sizes,
    index_ref,
    orders_ref,
    blocks_ref,
    state_ref,
    weights_ref,
    out_ref,
    body,
    tail,
    state_sems,
    out_body,
    out_tail,
    out_sems,
    xm,
    xe,
    lm,
    le,
    um,
    ue,
):
    levels, slot_count, slot_width, truncation, pair_count = sizes
    half = (truncation + 1) // 2
    parts = column_parts(state_ref.shape[1])
    head = state_ref.shape[0] - body.shape[0]
    copies = state_copies(state_ref, head, body, tail, state_sems)
    for copy in copies:
        copy.start()

    mask = edge_masks(slot_count, levels - LANES, (ROWS, LANES), 0)
    even = lax.broadcasted_iota(jnp.int32, (ROWS, LANES), 0) % 2 == 0

    def unfold(d, carry):
        for j in range(pair_count):
            n = index_ref[d * WORDS + j]
            block = blocks_ref[d * pair_count + j].astype(jnp.float32)
            edge = jnp.where(even, block[ROWS - 2 : ROWS - 1], block[ROWS - 1 :])
            edge = jnp.where(mask, edge, 0.0)
            start = UP * (half - 1 - n)
            low = LOW * n
            um[pl.ds(start, ROWS), :] = block
            ue[pl.ds(start, ROWS), :] = edge
            lm[pl.ds(low, 16), :] = block[:16]
            le[pl.ds(low, 16), :] = edge[:16]
        return carry

    lax.fori_loop(0, half // pair_count, unfold, 0, unroll=4)

    def regroup(k, carry):
        s = slot_count - 1 - k
        order = jnp.maximum(orders_ref[s], 0)
        base = FRONT + s * slot_width
        for p in range(2):
            for x, low, up in ((xm, lm, um), (xe, le, ue)):
                x[pl.ds(base + 2 * (half + 1) + p, half, stride=2), :] = up[
                    pl.ds(2 * s + p, half, stride=UP), :
                ]
                x[pl.ds(base - 2 * order + p, half, stride=2), :] = low[
                    pl.ds(2 * s + p, half, stride=LOW), :
                ]
                x[pl.ds(base + 2 * (half - order) + p, half, stride=2), :] = up[
                    pl.ds(2 * (slot_count + s) + p, half, stride=UP), :
                ]
            third = UP * (half - 1 - order) + 4 * slot_count + p
            place = base + 2 * (truncation + 1 - order) + p
            xm[pl.ds(place, 1), :] = um[pl.ds(third, 1), :]
            xe[pl.ds(place, 1), :] = ue[pl.ds(third, 1), :]
        return carry

    lax.fori_loop(0, slot_count, regroup, 0)

    row = lax.broadcasted_iota(jnp.int32, (state_ref.shape[0] - head, 1), 0)
    sends = []
    for k, (start, size) in enumerate(parts):
        copies[k].wait()
        at_end = k == len(parts) - 1
        base = tail[...] if at_end else body[:, start : start + size]
        lines = [x[pl.ds(FRONT + start, size), :] for x in (xm, xe)]
        moved = lax.dot_general(
            weights_ref[...],
            jnp.concatenate(lines, axis=1).astype(jnp.bfloat16),
            (((1,), (1,)), ((), ())),
            preferred_element_type=jnp.float32,
        )
        columns = start + lax.broadcasted_iota(jnp.int32, (1, size), 1)
        order, _ = slot_lines(columns, orders_ref, slot_count, slot_width)
        live = order >= 0
        kept = jnp.where(row >= levels - head, base.astype(jnp.float32), 0.0)
        first = jnp.where(live, moved[:head], 0.0).astype(jnp.bfloat16)
        second = jnp.where(live, kept + moved[head:], 0.0).astype(jnp.bfloat16)
        if at_end:
            out_tail[:head, :] = first
            out_tail[head:, :] = second
            source = out_tail
        else:
            out_body[:head, start : start + size] = first
            out_body[head:, start : start + size] = second
            source = out_body.at[:, pl.ds(start, size)]
        target = out_ref.at[:, pl.ds(start, size)]
        sends.append(pltpu.make_async_copy(source, target, out_sems.at[k]))
        sends[-1].start()
    for send in sends:
        send.wait()


def level_of_lane(levels, slot_count):
    edge = levels - LANES
    table = np.zeros((2 * LANES, levels), np.float32)
    table[np.arange(LANES), np.arange(LANES)] = 1.0
    folded = np.arange(edge * (2 * slot_count + 1))
    table[LANES + folded, LANES + folded % edge] = 1.0
    return table


def shards(
    state,
    held_orders,
    pair_lows,
    inverses,
    height_operator,
    pressure_column,
    thermal_response_matrix,
    mass_row,
):
    levels = height_operator.shape[0]
    pair_count = pair_lows.shape[0]
    slot_count = held_orders.shape[0]
    devices = lax.axis_size(GRP_WAVE)
    half = pair_count * devices
    truncation = 2 * half - 1
    slot_width = 2 * (truncation + 2)
    width = slot_count * slot_width
    rows = state.shape[0]
    parts = column_parts(width)
    split = parts[-1][0]
    bf16, f32 = jnp.bfloat16, jnp.float32
    vmem = pl.BlockSpec(memory_space=pltpu.VMEM)
    smem = pl.BlockSpec(memory_space=pltpu.SMEM)
    hbm = pl.BlockSpec(memory_space=pl.ANY)

    def params(mib):
        return pltpu.CompilerParams(vmem_limit_bytes=mib * 1024 * 1024)

    scratch = [
        pltpu.VMEM((FRONT + width + 6, LANES), f32),
        pltpu.VMEM((FRONT + width + 6, LANES), f32),
        pltpu.VMEM((LOW * half, LANES), f32),
        pltpu.VMEM((LOW * half, LANES), f32),
        pltpu.VMEM((UP * half, LANES), f32),
        pltpu.VMEM((UP * half, LANES), f32),
    ]

    own = jnp.concatenate([pair_lows, held_orders])
    own = jnp.pad(own, (0, LANES - own.shape[0]))
    index = lax.all_to_all(
        jnp.broadcast_to(own[None, None], (devices, 1, LANES)), GRP_WAVE, 0, 0, tiled=True
    ).reshape(devices, LANES)

    table = level_of_lane(levels, slot_count)
    padded = -(-levels // 16) * 16
    table = jnp.asarray(table, bf16)

    message = pl.pallas_call(
        functools.partial(rhs_kernel, (levels, slot_count, slot_width, truncation, pair_count)),
        in_specs=[
            hbm,
            smem,
            hbm,
            hbm,
            vmem,
        ],
        out_specs=hbm,
        out_shape=jax.ShapeDtypeStruct((half, ROWS, LANES), bf16),
        scratch_shapes=[
            pltpu.SMEM((devices, LANES), jnp.int32),
            pltpu.SemaphoreType.DMA,
            pltpu.VMEM((levels, levels), bf16),
            pltpu.SemaphoreType.DMA,
            pltpu.VMEM((padded, rows - LANES), bf16),
            pltpu.VMEM((rows, split), bf16),
            pltpu.VMEM((rows, width - split), bf16),
            pltpu.SemaphoreType.DMA((len(parts),)),
            pltpu.VMEM((half, ROWS, LANES), bf16),
            pltpu.SemaphoreType.DMA((PARTS,)),
        ]
        + scratch,
        compiler_params=params(56),
        name="right_side",
    )(index, held_orders, state, height_operator, pressure_column)

    arrived = lax.all_to_all(
        message.reshape(devices, pair_count * ROWS, LANES), GRP_WAVE, 0, 0, tiled=True
    ).reshape(devices, pair_count, ROWS, LANES)

    weights = jnp.einsum("al,jtkl->jtak", table, inverses, preferred_element_type=f32)
    weights = jnp.einsum("jtak,bk->jtab", weights.astype(bf16), table, preferred_element_type=f32)
    weights = weights.astype(bf16)
    words = index[:, :WORDS].reshape(-1)
    chunk = 32
    solved = pl.pallas_call(
        functools.partial(solve_kernel, (levels, slot_count, chunk)),
        in_specs=[smem, smem, vmem, hbm],
        out_specs=hbm,
        out_shape=jax.ShapeDtypeStruct((devices, pair_count, ROWS, LANES), bf16),
        scratch_shapes=[
            pltpu.VMEM((pair_count, 2, 2 * LANES, 2 * LANES), bf16),
            pltpu.SemaphoreType.DMA((pair_count,)),
            pltpu.VMEM((devices, pair_count, ROWS, LANES), bf16),
            pltpu.SemaphoreType.DMA((PARTS,)),
        ],
        compiler_params=params(24),
        name="solve",
    )(pair_lows, words, arrived, weights)

    returned = lax.all_to_all(
        solved.reshape(devices, pair_count * ROWS, LANES), GRP_WAVE, 0, 0, tiled=True
    ).reshape(half, ROWS, LANES)

    head = levels // 8 * 8
    response = jnp.concatenate(
        [jnp.eye(levels, dtype=bf16), -thermal_response_matrix, -mass_row[None, :]], axis=0
    )
    response = jnp.dot(response, table.T, preferred_element_type=f32).astype(bf16)
    return pl.pallas_call(
        functools.partial(final_kernel, (levels, slot_count, slot_width, truncation, pair_count)),
        in_specs=[smem, smem, vmem, hbm, vmem],
        out_specs=hbm,
        out_shape=jax.ShapeDtypeStruct((rows, width), bf16),
        scratch_shapes=[
            pltpu.VMEM((rows - head, split), bf16),
            pltpu.VMEM((rows - head, width - split), bf16),
            pltpu.SemaphoreType.DMA((len(parts),)),
            pltpu.VMEM((rows, split), bf16),
            pltpu.VMEM((rows, width - split), bf16),
            pltpu.SemaphoreType.DMA((len(parts),)),
        ]
        + scratch,
        compiler_params=params(48),
        name="final",
    )(words, held_orders, returned, state, response)


def solution(mesh):
    torus = Mesh(
        mesh.devices.reshape(mesh.shape["grp"], 4, 4, 2), ("grp", "wave_0", "wave_1", "wave_2")
    )
    placed = (
        P(None, GRP_WAVE),
        P(GRP_WAVE),
        P(GRP_WAVE),
        P(GRP_WAVE, None, None, None),
        P(),
        P(),
        P(),
        P(),
    )
    return jax.shard_map(
        shards, mesh=torus, in_specs=placed, out_specs=P(None, GRP_WAVE), check_vma=False
    )
```

```python
import functools

import jax
import jax.numpy as jnp
import numpy as np
from jax import lax
from jax.experimental import pallas as pl
from jax.experimental.pallas import tpu as pltpu
from jax.sharding import Mesh
from jax.sharding import PartitionSpec as P

GRP_WAVE = ("grp", "wave_0", "wave_1", "wave_2")

LANES = 128
ROWS = 24
FRONT = 768
WORDS = 8
TILE = 3840
PARTS = 4
BIG = 1 << 20
LOW = 17
UP = 25


def edge_masks(slot_count, edge, shape, row_dim):
    rows = lax.broadcasted_iota(jnp.int32, shape, row_dim)
    lanes = lax.broadcasted_iota(jnp.int32, shape, len(shape) - 1)
    group = rows >> 1
    return (lanes >= edge * group) & (lanes < edge * (group + 1)) & (rows < 4 * slot_count + 2)


def parity_fold(parts, axis):
    total = parts[0]
    for part in parts[1:]:
        total = total + part
    total = total + pltpu.roll(total, 2, axis)
    return total + pltpu.roll(total, 4, axis)


def slot_lines(columns, orders_ref, slot_count, slot_width):
    order = jnp.full(columns.shape, -1, jnp.int32)
    place = columns
    for s in range(slot_count):
        inside = (columns >= s * slot_width) & (columns < (s + 1) * slot_width)
        order = jnp.where(inside, orders_ref[s], order)
        place = jnp.where(inside, columns - s * slot_width, place)
    return order, place // 2


def column_parts(width):
    starts = list(range(0, width - TILE // 2, TILE))
    return [(a, b - a) for a, b in zip(starts, starts[1:] + [width])]


def state_copies(state_ref, first, body, tail, sems):
    copies = []
    parts = column_parts(state_ref.shape[1])
    for k, (start, size) in enumerate(parts):
        source = state_ref.at[pl.ds(first, body.shape[0]), pl.ds(start, size)]
        target = tail if k == len(parts) - 1 else body.at[:, pl.ds(start, size)]
        copies.append(pltpu.make_async_copy(source, target, sems.at[k]))
    return copies


def rhs_kernel(
    sizes,
    index_ref,
    orders_ref,
    state_ref,
    height_ref,
    pressure_ref,
    out_ref,
    near,
    index_sem,
    height,
    height_sem,
    drive,
    body,
    tail,
    state_sems,
    stage,
    out_sems,
    xm,
    xe,
    lm,
    le,
    um,
    ue,
):
    levels, slot_count, slot_width, truncation, pair_count = sizes
    half = (truncation + 1) // 2
    parts = column_parts(state_ref.shape[1])
    bring = pltpu.make_async_copy(height_ref, height, height_sem)
    bring.start()
    copies = state_copies(state_ref, 0, body, tail, state_sems)
    for copy in copies:
        copy.start()
    fetch = pltpu.make_async_copy(index_ref, near, index_sem)
    fetch.start()

    edge_count = levels - LANES
    lane = lax.broadcasted_iota(jnp.int32, (LANES, drive.shape[0] - LANES), 0)
    group = jnp.zeros_like(lane)
    for g in range(1, 2 * slot_count + 2):
        group = group + jnp.where(lane >= edge_count * g, 1, 0)
    wanted = lax.broadcasted_iota(jnp.int32, lane.shape, 1) == lane - edge_count * group
    spread = jnp.where(wanted & (group <= 2 * slot_count), 1.0, 0.0).astype(jnp.bfloat16)
    column = jnp.broadcast_to(pressure_ref[...].reshape(1, levels).astype(jnp.float32), (8, levels))
    column = jnp.transpose(column)[:, :1]
    drive[...] = jnp.zeros_like(drive)
    last = drive.shape[1] - 1
    drive[:levels, last:] = column.astype(jnp.bfloat16)
    bring.wait()
    drive[:levels, last - levels : last] = height[...]
    padded = drive.shape[0]

    for k, (start, size) in enumerate(parts):
        copies[k].wait()
        if k == len(parts) - 1:
            upper, lower = tail[:padded, :], tail[LANES:, :]
        else:
            upper = body[:padded, start : start + size]
            lower = body[LANES:, start : start + size]
        columns = start + lax.broadcasted_iota(jnp.int32, (1, size), 1)
        order, coeff = slot_lines(columns, orders_ref, slot_count, slot_width)
        degree = jnp.where(coeff <= truncation - order, order + coeff, coeff - 1)
        lap = (degree * (degree + 1)).astype(jnp.float32) / float(truncation * (truncation + 1))
        pull = jnp.dot(drive[...], lower, preferred_element_type=jnp.float32)
        right = (upper.astype(jnp.float32) + lap * pull).astype(jnp.bfloat16)
        xm[pl.ds(FRONT + start, size), :] = jnp.transpose(right[:LANES].astype(jnp.float32))
        xe[pl.ds(FRONT + start, size), :] = lax.dot_general(
            jnp.transpose(right[LANES:].astype(jnp.float32)).astype(jnp.bfloat16),
            spread,
            (((1,), (1,)), ((), ())),
            preferred_element_type=jnp.float32,
        )

    def regroup(s, carry):
        order = jnp.maximum(orders_ref[s], 0)
        base = FRONT + s * slot_width
        for p in range(2):
            for x, low, up in ((xm, lm, um), (xe, le, ue)):
                up[pl.ds(2 * s + p, half, stride=UP), :] = x[
                    pl.ds(base + 2 * (half + 1) + p, half, stride=2), :
                ]
                low[pl.ds(2 * s + p, half, stride=LOW), :] = x[
                    pl.ds(base - 2 * order + p, half, stride=2), :
                ]
                up[pl.ds(2 * (slot_count + s) + p, half, stride=UP), :] = x[
                    pl.ds(base + 2 * (half - order) + p, half, stride=2), :
                ]

                @pl.when(orders_ref[s] >= 0)
                def _(x=x, up=up, p=p):
                    third = UP * (half - 1 - order) + 4 * slot_count + p
                    up[pl.ds(third, 1), :] = x[
                        pl.ds(base + 2 * (truncation + 1 - order) + p, 1), :
                    ]

        return carry

    lax.fori_loop(0, slot_count, regroup, 0)

    row = lax.broadcasted_iota(jnp.int32, (16, LANES), 0)
    order_rows = jnp.full((16, LANES), BIG, jnp.int32)
    for s in range(slot_count):
        order_rows = jnp.where(row // 2 == s, jnp.maximum(orders_ref[s], 0), order_rows)
    mask = edge_masks(slot_count, levels - LANES, (ROWS, LANES), 0)
    bottom = lax.broadcasted_iota(jnp.int32, (8, LANES), 0) >= 6

    def assemble(d, j):
        n = near[d, j]
        start = UP * (half - 1 - n)
        low = LOW * n
        lines = um[pl.ds(start, ROWS), :]
        edge = ue[pl.ds(start, ROWS), :]
        own = order_rows <= n
        top = jnp.where(own, lm[pl.ds(low, 16), :], lines[:16])
        top_edge = jnp.where(own, le[pl.ds(low, 16), :], edge[:16])
        folded = parity_fold(
            [
                jnp.where(mask[:8], top_edge[:8], 0.0),
                jnp.where(mask[8:16], top_edge[8:], 0.0),
                jnp.where(mask[16:], edge[16:], 0.0),
            ],
            0,
        )
        block = jnp.concatenate([top, jnp.where(bottom, folded, lines[16:])], axis=0)
        stage[d * pair_count + j] = block.astype(jnp.bfloat16)

    fetch.wait()
    count = half // pair_count // PARTS
    sends = []
    for k in range(PARTS):

        def assemble_all(d, carry):
            for j in range(pair_count):
                assemble(d, j)
            return carry

        lax.fori_loop(k * count, (k + 1) * count, assemble_all, 0, unroll=4)
        some = pl.ds(k * count * pair_count, count * pair_count)
        sends.append(pltpu.make_async_copy(stage.at[some], out_ref.at[some], out_sems.at[k]))
        sends[-1].start()
    for send in sends:
        send.wait()


def solve_kernel(sizes, lows_ref, index_ref, blocks_ref, weights_ref, out_ref):
    levels, slot_count = sizes
    count, pair_count = blocks_ref.shape[0], blocks_ref.shape[1]
    shape = (count, ROWS, LANES)
    mask = edge_masks(slot_count, levels - LANES, (ROWS, LANES), 0)[None]
    even = (lax.broadcasted_iota(jnp.int32, (ROWS, LANES), 0) & 1 == 0)[None]
    bottom = (lax.broadcasted_iota(jnp.int32, (8, LANES), 0) >= 6)[None]
    slot = lax.broadcasted_iota(jnp.int32, (16, LANES), 0) >> 1
    orders = []
    for k in range(count):
        lines = jnp.full((16, LANES), BIG, jnp.int32)
        for s in range(slot_count):
            order = index_ref[(pl.program_id(0) * count + k) * WORDS + pair_count + s]
            lines = jnp.where(slot == s, order, lines)
        orders.append(lines)
    orders = jnp.stack(orders)
    for j in range(pair_count):
        body = blocks_ref[:, j].astype(jnp.float32)
        edge = jnp.where(even, body[:, ROWS - 2 : ROWS - 1], body[:, ROWS - 1 :])
        edge = jnp.where(mask, edge, 0.0)
        lines = jnp.concatenate([body, edge], axis=-1)
        top = lines[:, :16].reshape(count * 16, 2 * LANES).astype(jnp.bfloat16)
        lines = lines.reshape(count * ROWS, 2 * LANES).astype(jnp.bfloat16)
        upper = jnp.dot(lines, weights_ref[j, 1], preferred_element_type=jnp.float32)
        upper = upper.reshape(count, ROWS, 2 * LANES)
        lower = jnp.dot(top, weights_ref[j, 0], preferred_element_type=jnp.float32)
        lower = lower.reshape(count, 16, 2 * LANES)
        own = orders <= lows_ref[j]
        main = jnp.where(own, lower[..., :LANES], upper[:, :16, :LANES])
        edge = jnp.where(own, lower[..., LANES:], upper[:, :16, LANES:])
        edge = jnp.where(mask[:, :16], edge, 0.0)
        rest = jnp.where(mask[:, 16:], upper[:, 16:, LANES:], 0.0)
        folded = parity_fold([edge[:, :8], edge[:, 8:], rest], 1)
        rest = jnp.where(bottom, folded, upper[:, 16:, :LANES])
        out_ref[:, j] = jnp.concatenate([main, rest], axis=1).astype(jnp.bfloat16)


def final_kernel(
    sizes,
    index_ref,
    orders_ref,
    blocks_ref,
    state_ref,
    weights_ref,
    out_ref,
    body,
    tail,
    state_sems,
    out_body,
    out_tail,
    out_sems,
    xm,
    xe,
    lm,
    le,
    um,
    ue,
):
    levels, slot_count, slot_width, truncation, pair_count = sizes
    half = (truncation + 1) // 2
    parts = column_parts(state_ref.shape[1])
    head = state_ref.shape[0] - body.shape[0]
    copies = state_copies(state_ref, head, body, tail, state_sems)
    for copy in copies:
        copy.start()

    mask = edge_masks(slot_count, levels - LANES, (ROWS, LANES), 0)
    even = lax.broadcasted_iota(jnp.int32, (ROWS, LANES), 0) % 2 == 0

    def unfold(d, carry):
        for j in range(pair_count):
            n = index_ref[d * WORDS + j]
            block = blocks_ref[d * pair_count + j].astype(jnp.float32)
            edge = jnp.where(even, block[ROWS - 2 : ROWS - 1], block[ROWS - 1 :])
            edge = jnp.where(mask, edge, 0.0)
            start = UP * (half - 1 - n)
            low = LOW * n
            um[pl.ds(start, ROWS), :] = block
            ue[pl.ds(start, ROWS), :] = edge
            lm[pl.ds(low, 16), :] = block[:16]
            le[pl.ds(low, 16), :] = edge[:16]
        return carry

    lax.fori_loop(0, half // pair_count, unfold, 0, unroll=4)

    def regroup(k, carry):
        s = slot_count - 1 - k
        order = jnp.maximum(orders_ref[s], 0)
        base = FRONT + s * slot_width
        for p in range(2):
            for x, low, up in ((xm, lm, um), (xe, le, ue)):
                x[pl.ds(base + 2 * (half + 1) + p, half, stride=2), :] = up[
                    pl.ds(2 * s + p, half, stride=UP), :
                ]
                x[pl.ds(base - 2 * order + p, half, stride=2), :] = low[
                    pl.ds(2 * s + p, half, stride=LOW), :
                ]
                x[pl.ds(base + 2 * (half - order) + p, half, stride=2), :] = up[
                    pl.ds(2 * (slot_count + s) + p, half, stride=UP), :
                ]
            third = UP * (half - 1 - order) + 4 * slot_count + p
            place = base + 2 * (truncation + 1 - order) + p
            xm[pl.ds(place, 1), :] = um[pl.ds(third, 1), :]
            xe[pl.ds(place, 1), :] = ue[pl.ds(third, 1), :]
        return carry

    lax.fori_loop(0, slot_count, regroup, 0)

    row = lax.broadcasted_iota(jnp.int32, (state_ref.shape[0] - head, 1), 0)
    sends = []
    for k, (start, size) in enumerate(parts):
        copies[k].wait()
        at_end = k == len(parts) - 1
        base = tail[...] if at_end else body[:, start : start + size]
        lines = [x[pl.ds(FRONT + start, size), :] for x in (xm, xe)]
        moved = lax.dot_general(
            weights_ref[...],
            jnp.concatenate(lines, axis=1).astype(jnp.bfloat16),
            (((1,), (1,)), ((), ())),
            preferred_element_type=jnp.float32,
        )
        columns = start + lax.broadcasted_iota(jnp.int32, (1, size), 1)
        order, _ = slot_lines(columns, orders_ref, slot_count, slot_width)
        live = order >= 0
        kept = jnp.where(row >= levels - head, base.astype(jnp.float32), 0.0)
        first = jnp.where(live, moved[:head], 0.0).astype(jnp.bfloat16)
        second = jnp.where(live, kept + moved[head:], 0.0).astype(jnp.bfloat16)
        if at_end:
            out_tail[:head, :] = first
            out_tail[head:, :] = second
            source = out_tail
        else:
            out_body[:head, start : start + size] = first
            out_body[head:, start : start + size] = second
            source = out_body.at[:, pl.ds(start, size)]
        target = out_ref.at[:, pl.ds(start, size)]
        sends.append(pltpu.make_async_copy(source, target, out_sems.at[k]))
        sends[-1].start()
    for send in sends:
        send.wait()


def level_of_lane(levels, slot_count):
    edge = levels - LANES
    table = np.zeros((2 * LANES, levels), np.float32)
    table[np.arange(LANES), np.arange(LANES)] = 1.0
    folded = np.arange(edge * (2 * slot_count + 1))
    table[LANES + folded, LANES + folded % edge] = 1.0
    return table


def shards(
    state,
    held_orders,
    pair_lows,
    inverses,
    height_operator,
    pressure_column,
    thermal_response_matrix,
    mass_row,
):
    levels = height_operator.shape[0]
    pair_count = pair_lows.shape[0]
    slot_count = held_orders.shape[0]
    devices = lax.axis_size(GRP_WAVE)
    half = pair_count * devices
    truncation = 2 * half - 1
    slot_width = 2 * (truncation + 2)
    width = slot_count * slot_width
    rows = state.shape[0]
    parts = column_parts(width)
    split = parts[-1][0]
    bf16, f32 = jnp.bfloat16, jnp.float32
    vmem = pl.BlockSpec(memory_space=pltpu.VMEM)
    smem = pl.BlockSpec(memory_space=pltpu.SMEM)
    hbm = pl.BlockSpec(memory_space=pl.ANY)

    def params(mib):
        return pltpu.CompilerParams(vmem_limit_bytes=mib * 1024 * 1024)

    scratch = [
        pltpu.VMEM((FRONT + width + 6, LANES), f32),
        pltpu.VMEM((FRONT + width + 6, LANES), f32),
        pltpu.VMEM((LOW * half, LANES), f32),
        pltpu.VMEM((LOW * half, LANES), f32),
        pltpu.VMEM((UP * half, LANES), f32),
        pltpu.VMEM((UP * half, LANES), f32),
    ]

    own = jnp.concatenate([pair_lows, held_orders])
    own = jnp.pad(own, (0, LANES - own.shape[0]))
    index = lax.all_to_all(
        jnp.broadcast_to(own[None, None], (devices, 1, LANES)), GRP_WAVE, 0, 0, tiled=True
    ).reshape(devices, LANES)

    table = level_of_lane(levels, slot_count)
    padded = -(-levels // 16) * 16
    table = jnp.asarray(table, bf16)

    message = pl.pallas_call(
        functools.partial(rhs_kernel, (levels, slot_count, slot_width, truncation, pair_count)),
        in_specs=[
            hbm,
            smem,
            hbm,
            hbm,
            vmem,
        ],
        out_specs=hbm,
        out_shape=jax.ShapeDtypeStruct((half, ROWS, LANES), bf16),
        scratch_shapes=[
            pltpu.SMEM((devices, LANES), jnp.int32),
            pltpu.SemaphoreType.DMA,
            pltpu.VMEM((levels, levels), bf16),
            pltpu.SemaphoreType.DMA,
            pltpu.VMEM((padded, rows - LANES), bf16),
            pltpu.VMEM((rows, split), bf16),
            pltpu.VMEM((rows, width - split), bf16),
            pltpu.SemaphoreType.DMA((len(parts),)),
            pltpu.VMEM((half, ROWS, LANES), bf16),
            pltpu.SemaphoreType.DMA((PARTS,)),
        ]
        + scratch,
        compiler_params=params(56),
        name="right_side",
    )(index, held_orders, state, height_operator, pressure_column)

    arrived = lax.all_to_all(
        message.reshape(devices, pair_count * ROWS, LANES), GRP_WAVE, 0, 0, tiled=True
    ).reshape(devices, pair_count, ROWS, LANES)

    weights = jnp.einsum("al,jtkl->jtak", table, inverses, preferred_element_type=f32)
    weights = jnp.einsum("jtak,bk->jtab", weights.astype(bf16), table, preferred_element_type=f32)
    weights = weights.astype(bf16)
    words = index[:, :WORDS].reshape(-1)
    chunk = 64
    solved = pl.pallas_call(
        functools.partial(solve_kernel, (levels, slot_count)),
        grid=(devices // chunk,),
        in_specs=[
            smem,
            smem,
            pl.BlockSpec((chunk, pair_count, ROWS, LANES), lambda i: (i, 0, 0, 0)),
            vmem,
        ],
        out_specs=pl.BlockSpec((chunk, pair_count, ROWS, LANES), lambda i: (i, 0, 0, 0)),
        out_shape=jax.ShapeDtypeStruct((devices, pair_count, ROWS, LANES), bf16),
        compiler_params=params(52),
        name="solve",
    )(pair_lows, words, arrived, weights)

    returned = lax.all_to_all(
        solved.reshape(devices, pair_count * ROWS, LANES), GRP_WAVE, 0, 0, tiled=True
    ).reshape(half, ROWS, LANES)

    head = levels // 8 * 8
    response = jnp.concatenate(
        [jnp.eye(levels, dtype=bf16), -thermal_response_matrix, -mass_row[None, :]], axis=0
    )
    response = jnp.dot(response, table.T, preferred_element_type=f32).astype(bf16)
    return pl.pallas_call(
        functools.partial(final_kernel, (levels, slot_count, slot_width, truncation, pair_count)),
        in_specs=[smem, smem, vmem, hbm, vmem],
        out_specs=hbm,
        out_shape=jax.ShapeDtypeStruct((rows, width), bf16),
        scratch_shapes=[
            pltpu.VMEM((rows - head, split), bf16),
            pltpu.VMEM((rows - head, width - split), bf16),
            pltpu.SemaphoreType.DMA((len(parts),)),
            pltpu.VMEM((rows, split), bf16),
            pltpu.VMEM((rows, width - split), bf16),
            pltpu.SemaphoreType.DMA((len(parts),)),
        ]
        + scratch,
        compiler_params=params(48),
        name="final",
    )(words, held_orders, returned, state, response)


def solution(mesh):
    torus = Mesh(
        mesh.devices.reshape(mesh.shape["grp"], 4, 4, 2), ("grp", "wave_0", "wave_1", "wave_2")
    )
    placed = (
        P(None, GRP_WAVE),
        P(GRP_WAVE),
        P(GRP_WAVE),
        P(GRP_WAVE, None, None, None),
        P(),
        P(),
        P(),
        P(),
    )
    return jax.shard_map(
        shards, mesh=torus, in_specs=placed, out_specs=P(None, GRP_WAVE), check_vma=False
    )
```

```python
import functools

import jax
import jax.numpy as jnp
import numpy as np
from jax import lax
from jax.experimental import pallas as pl
from jax.experimental.pallas import tpu as pltpu
from jax.sharding import Mesh
from jax.sharding import PartitionSpec as P

GRP_WAVE = ("grp", "wave_0", "wave_1", "wave_2")

LANES = 128
ROWS = 24
FRONT = 768
WORDS = 8
TILE = 3840
PARTS = 4
BIG = 1 << 20
LOW = 17
UP = 25


def edge_masks(slot_count, edge, shape, row_dim):
    rows = lax.broadcasted_iota(jnp.int32, shape, row_dim)
    lanes = lax.broadcasted_iota(jnp.int32, shape, len(shape) - 1)
    group = rows // 2
    return (lanes >= edge * group) & (lanes < edge * (group + 1)) & (rows < 4 * slot_count + 2)


def parity_fold(parts, axis):
    total = parts[0]
    for part in parts[1:]:
        total = total + part
    total = total + pltpu.roll(total, 2, axis)
    return total + pltpu.roll(total, 4, axis)


def slot_lines(columns, orders_ref, slot_count, slot_width):
    order = jnp.full(columns.shape, -1, jnp.int32)
    place = columns
    for s in range(slot_count):
        inside = (columns >= s * slot_width) & (columns < (s + 1) * slot_width)
        order = jnp.where(inside, orders_ref[s], order)
        place = jnp.where(inside, columns - s * slot_width, place)
    return order, place // 2


def column_parts(width):
    starts = list(range(0, width - TILE // 2, TILE))
    return [(a, b - a) for a, b in zip(starts, starts[1:] + [width])]


def state_copies(state_ref, first, body, tail, sems):
    copies = []
    parts = column_parts(state_ref.shape[1])
    for k, (start, size) in enumerate(parts):
        source = state_ref.at[pl.ds(first, body.shape[0]), pl.ds(start, size)]
        target = tail if k == len(parts) - 1 else body.at[:, pl.ds(start, size)]
        copies.append(pltpu.make_async_copy(source, target, sems.at[k]))
    return copies


def rhs_kernel(
    sizes,
    index_ref,
    orders_ref,
    state_ref,
    height_ref,
    pressure_ref,
    out_ref,
    near,
    index_sem,
    height,
    height_sem,
    drive,
    body,
    tail,
    state_sems,
    stage,
    out_sems,
    xm,
    xe,
    lm,
    le,
    um,
    ue,
):
    levels, slot_count, slot_width, truncation, pair_count = sizes
    half = (truncation + 1) // 2
    parts = column_parts(state_ref.shape[1])
    bring = pltpu.make_async_copy(height_ref, height, height_sem)
    bring.start()
    copies = state_copies(state_ref, 0, body, tail, state_sems)
    for copy in copies:
        copy.start()
    fetch = pltpu.make_async_copy(index_ref, near, index_sem)
    fetch.start()

    edge_count = levels - LANES
    lane = lax.broadcasted_iota(jnp.int32, (LANES, drive.shape[0] - LANES), 0)
    group = jnp.zeros_like(lane)
    for g in range(1, 2 * slot_count + 2):
        group = group + jnp.where(lane >= edge_count * g, 1, 0)
    wanted = lax.broadcasted_iota(jnp.int32, lane.shape, 1) == lane - edge_count * group
    spread = jnp.where(wanted & (group <= 2 * slot_count), 1.0, 0.0).astype(jnp.bfloat16)
    column = jnp.broadcast_to(pressure_ref[...].reshape(1, levels).astype(jnp.float32), (8, levels))
    column = jnp.transpose(column)[:, :1]
    drive[...] = jnp.zeros_like(drive)
    last = drive.shape[1] - 1
    drive[:levels, last:] = column.astype(jnp.bfloat16)
    bring.wait()
    drive[:levels, last - levels : last] = height[...]
    padded = drive.shape[0]

    for k, (start, size) in enumerate(parts):
        copies[k].wait()
        if k == len(parts) - 1:
            upper, lower = tail[:padded, :], tail[LANES:, :]
        else:
            upper = body[:padded, start : start + size]
            lower = body[LANES:, start : start + size]
        columns = start + lax.broadcasted_iota(jnp.int32, (1, size), 1)
        order, coeff = slot_lines(columns, orders_ref, slot_count, slot_width)
        degree = jnp.where(coeff <= truncation - order, order + coeff, coeff - 1)
        lap = (degree * (degree + 1)).astype(jnp.float32) / float(truncation * (truncation + 1))
        pull = jnp.dot(drive[...], lower, preferred_element_type=jnp.float32)
        right = (upper.astype(jnp.float32) + lap * pull).astype(jnp.bfloat16)
        xm[pl.ds(FRONT + start, size), :] = jnp.transpose(right[:LANES].astype(jnp.float32))
        xe[pl.ds(FRONT + start, size), :] = lax.dot_general(
            jnp.transpose(right[LANES:].astype(jnp.float32)).astype(jnp.bfloat16),
            spread,
            (((1,), (1,)), ((), ())),
            preferred_element_type=jnp.float32,
        )

    def regroup(s, carry):
        order = jnp.maximum(orders_ref[s], 0)
        base = FRONT + s * slot_width
        for p in range(2):
            for x, low, up in ((xm, lm, um), (xe, le, ue)):
                up[pl.ds(2 * s + p, half, stride=UP), :] = x[
                    pl.ds(base + 2 * (half + 1) + p, half, stride=2), :
                ]
                low[pl.ds(2 * s + p, half, stride=LOW), :] = x[
                    pl.ds(base - 2 * order + p, half, stride=2), :
                ]
                up[pl.ds(2 * (slot_count + s) + p, half, stride=UP), :] = x[
                    pl.ds(base + 2 * (half - order) + p, half, stride=2), :
                ]

                @pl.when(orders_ref[s] >= 0)
                def _(x=x, up=up, p=p):
                    third = UP * (half - 1 - order) + 4 * slot_count + p
                    up[pl.ds(third, 1), :] = x[
                        pl.ds(base + 2 * (truncation + 1 - order) + p, 1), :
                    ]

        return carry

    lax.fori_loop(0, slot_count, regroup, 0)

    row = lax.broadcasted_iota(jnp.int32, (16, LANES), 0)
    order_rows = jnp.full((16, LANES), BIG, jnp.int32)
    for s in range(slot_count):
        order_rows = jnp.where(row // 2 == s, jnp.maximum(orders_ref[s], 0), order_rows)
    mask = edge_masks(slot_count, levels - LANES, (ROWS, LANES), 0)
    bottom = lax.broadcasted_iota(jnp.int32, (8, LANES), 0) >= 6

    def assemble(d, j):
        n = near[d, j]
        start = UP * (half - 1 - n)
        low = LOW * n
        lines = um[pl.ds(start, ROWS), :]
        edge = ue[pl.ds(start, ROWS), :]
        own = order_rows <= n
        top = jnp.where(own, lm[pl.ds(low, 16), :], lines[:16])
        top_edge = jnp.where(own, le[pl.ds(low, 16), :], edge[:16])
        folded = parity_fold(
            [
                jnp.where(mask[:8], top_edge[:8], 0.0),
                jnp.where(mask[8:16], top_edge[8:], 0.0),
                jnp.where(mask[16:], edge[16:], 0.0),
            ],
            0,
        )
        block = jnp.concatenate([top, jnp.where(bottom, folded, lines[16:])], axis=0)
        stage[d * pair_count + j] = block.astype(jnp.bfloat16)

    fetch.wait()
    count = half // pair_count // PARTS
    sends = []
    for k in range(PARTS):

        def assemble_all(d, carry):
            for j in range(pair_count):
                assemble(d, j)
            return carry

        lax.fori_loop(k * count, (k + 1) * count, assemble_all, 0, unroll=4)
        some = pl.ds(k * count * pair_count, count * pair_count)
        sends.append(pltpu.make_async_copy(stage.at[some], out_ref.at[some], out_sems.at[k]))
        sends[-1].start()
    for send in sends:
        send.wait()


def solve_kernel(
    sizes, lows_ref, index_ref, blocks_ref, weights_ref, out_ref, stage, out_sems
):
    levels, slot_count, chunk = sizes
    devices, pair_count = blocks_ref.shape[0], blocks_ref.shape[1]
    shape = (chunk, ROWS, LANES)
    mask = edge_masks(slot_count, levels - LANES, shape, 1)
    row = lax.broadcasted_iota(jnp.int32, shape, 1)
    slot = lax.broadcasted_iota(jnp.int32, (16, LANES), 0) // 2
    depth = weights_ref.shape[2]
    empty = jnp.zeros((2 * LANES - depth, 2 * LANES), jnp.bfloat16)

    def whole(j, t):
        return jnp.concatenate([weights_ref[j, t], empty], axis=0)

    def solve_some(first):
        orders = []
        for k in range(chunk):
            lines = jnp.full((16, LANES), BIG, jnp.int32)
            for s in range(slot_count):
                order = index_ref[(first + k) * WORDS + pair_count + s]
                lines = jnp.where(slot == s, order, lines)
            orders.append(lines)
        orders = jnp.stack(orders)
        here = pl.ds(first, chunk)
        for j in range(pair_count):
            body = blocks_ref[here, j].astype(jnp.float32)
            edge = jnp.where(row % 2 == 0, body[:, ROWS - 2 : ROWS - 1], body[:, ROWS - 1 :])
            edge = jnp.where(mask, edge, 0.0)
            lines = jnp.concatenate([body, edge], axis=-1)
            top = lines[:, :16].reshape(chunk * 16, 2 * LANES).astype(jnp.bfloat16)
            lines = lines.reshape(chunk * ROWS, 2 * LANES).astype(jnp.bfloat16)
            upper = jnp.dot(lines, whole(j, 1), preferred_element_type=jnp.float32)
            upper = upper.reshape(chunk, ROWS, 2 * LANES)
            lower = jnp.dot(top, whole(j, 0), preferred_element_type=jnp.float32)
            lower = lower.reshape(chunk, 16, 2 * LANES)
            own = orders <= lows_ref[j]
            main = jnp.where(own, lower[..., :LANES], upper[:, :16, :LANES])
            edge = jnp.where(own, lower[..., LANES:], upper[:, :16, LANES:])
            edge = jnp.where(mask[:, :16], edge, 0.0)
            rest = jnp.where(mask[:, 16:], upper[:, 16:, LANES:], 0.0)
            folded = parity_fold([edge[:, :8], edge[:, 8:], rest], 1)
            rest = jnp.where(row[:, 16:] >= ROWS - 2, folded, upper[:, 16:, :LANES])
            stage[here, j] = jnp.concatenate([main, rest], axis=1).astype(jnp.bfloat16)

    count = devices // PARTS
    sends = []
    for k in range(PARTS):

        def solve_all(c, carry):
            solve_some(k * count + c * chunk)
            return carry

        lax.fori_loop(0, count // chunk, solve_all, 0)
        some = pl.ds(k * count, count)
        sends.append(pltpu.make_async_copy(stage.at[some], out_ref.at[some], out_sems.at[k]))
        sends[-1].start()
    for send in sends:
        send.wait()


def final_kernel(
    sizes,
    index_ref,
    orders_ref,
    blocks_ref,
    state_ref,
    weights_ref,
    out_ref,
    body,
    tail,
    state_sems,
    out_body,
    out_tail,
    out_sems,
    xm,
    xe,
    lm,
    le,
    um,
    ue,
):
    levels, slot_count, slot_width, truncation, pair_count = sizes
    half = (truncation + 1) // 2
    parts = column_parts(state_ref.shape[1])
    head = state_ref.shape[0] - body.shape[0]
    copies = state_copies(state_ref, head, body, tail, state_sems)
    for copy in copies:
        copy.start()

    mask = edge_masks(slot_count, levels - LANES, (ROWS, LANES), 0)
    even = lax.broadcasted_iota(jnp.int32, (ROWS, LANES), 0) % 2 == 0

    def unfold(d, carry):
        for j in range(pair_count):
            n = index_ref[d * WORDS + j]
            block = blocks_ref[d * pair_count + j].astype(jnp.float32)
            edge = jnp.where(even, block[ROWS - 2 : ROWS - 1], block[ROWS - 1 :])
            edge = jnp.where(mask, edge, 0.0)
            start = UP * (half - 1 - n)
            low = LOW * n
            um[pl.ds(start, ROWS), :] = block
            ue[pl.ds(start, ROWS), :] = edge
            lm[pl.ds(low, 16), :] = block[:16]
            le[pl.ds(low, 16), :] = edge[:16]
        return carry

    lax.fori_loop(0, half // pair_count, unfold, 0, unroll=4)

    def regroup(k, carry):
        s = slot_count - 1 - k
        order = jnp.maximum(orders_ref[s], 0)
        base = FRONT + s * slot_width
        for p in range(2):
            for x, low, up in ((xm, lm, um), (xe, le, ue)):
                x[pl.ds(base + 2 * (half + 1) + p, half, stride=2), :] = up[
                    pl.ds(2 * s + p, half, stride=UP), :
                ]
                x[pl.ds(base - 2 * order + p, half, stride=2), :] = low[
                    pl.ds(2 * s + p, half, stride=LOW), :
                ]
                x[pl.ds(base + 2 * (half - order) + p, half, stride=2), :] = up[
                    pl.ds(2 * (slot_count + s) + p, half, stride=UP), :
                ]
            third = UP * (half - 1 - order) + 4 * slot_count + p
            place = base + 2 * (truncation + 1 - order) + p
            xm[pl.ds(place, 1), :] = um[pl.ds(third, 1), :]
            xe[pl.ds(place, 1), :] = ue[pl.ds(third, 1), :]
        return carry

    lax.fori_loop(0, slot_count, regroup, 0)

    row = lax.broadcasted_iota(jnp.int32, (state_ref.shape[0] - head, 1), 0)
    sends = []
    for k, (start, size) in enumerate(parts):
        copies[k].wait()
        at_end = k == len(parts) - 1
        base = tail[...] if at_end else body[:, start : start + size]
        lines = [x[pl.ds(FRONT + start, size), :] for x in (xm, xe)]
        moved = lax.dot_general(
            weights_ref[...],
            jnp.concatenate(lines, axis=1).astype(jnp.bfloat16),
            (((1,), (1,)), ((), ())),
            preferred_element_type=jnp.float32,
        )
        columns = start + lax.broadcasted_iota(jnp.int32, (1, size), 1)
        order, _ = slot_lines(columns, orders_ref, slot_count, slot_width)
        live = order >= 0
        kept = jnp.where(row >= levels - head, base.astype(jnp.float32), 0.0)
        first = jnp.where(live, moved[:head], 0.0).astype(jnp.bfloat16)
        second = jnp.where(live, kept + moved[head:], 0.0).astype(jnp.bfloat16)
        if at_end:
            out_tail[:head, :] = first
            out_tail[head:, :] = second
            source = out_tail
        else:
            out_body[:head, start : start + size] = first
            out_body[head:, start : start + size] = second
            source = out_body.at[:, pl.ds(start, size)]
        target = out_ref.at[:, pl.ds(start, size)]
        sends.append(pltpu.make_async_copy(source, target, out_sems.at[k]))
        sends[-1].start()
    for send in sends:
        send.wait()


def level_of_lane(levels, slot_count):
    edge = levels - LANES
    table = np.zeros((2 * LANES, levels), np.float32)
    table[np.arange(LANES), np.arange(LANES)] = 1.0
    folded = np.arange(edge * (2 * slot_count + 1))
    table[LANES + folded, LANES + folded % edge] = 1.0
    return table


def shards(
    state,
    held_orders,
    pair_lows,
    inverses,
    height_operator,
    pressure_column,
    thermal_response_matrix,
    mass_row,
):
    levels = height_operator.shape[0]
    pair_count = pair_lows.shape[0]
    slot_count = held_orders.shape[0]
    devices = lax.axis_size(GRP_WAVE)
    half = pair_count * devices
    truncation = 2 * half - 1
    slot_width = 2 * (truncation + 2)
    width = slot_count * slot_width
    rows = state.shape[0]
    parts = column_parts(width)
    split = parts[-1][0]
    bf16, f32 = jnp.bfloat16, jnp.float32
    vmem = pl.BlockSpec(memory_space=pltpu.VMEM)
    smem = pl.BlockSpec(memory_space=pltpu.SMEM)
    hbm = pl.BlockSpec(memory_space=pl.ANY)

    def params(mib):
        return pltpu.CompilerParams(vmem_limit_bytes=mib * 1024 * 1024)

    scratch = [
        pltpu.VMEM((FRONT + width + 6, LANES), f32),
        pltpu.VMEM((FRONT + width + 6, LANES), f32),
        pltpu.VMEM((LOW * half, LANES), f32),
        pltpu.VMEM((LOW * half, LANES), f32),
        pltpu.VMEM((UP * half, LANES), f32),
        pltpu.VMEM((UP * half, LANES), f32),
    ]

    own = jnp.concatenate([pair_lows, held_orders])
    own = jnp.pad(own, (0, LANES - own.shape[0]))
    index = lax.all_to_all(
        jnp.broadcast_to(own[None, None], (devices, 1, LANES)), GRP_WAVE, 0, 0, tiled=True
    ).reshape(devices, LANES)

    table = level_of_lane(levels, slot_count)
    padded = -(-levels // 16) * 16
    table = jnp.asarray(table, bf16)

    message = pl.pallas_call(
        functools.partial(rhs_kernel, (levels, slot_count, slot_width, truncation, pair_count)),
        in_specs=[
            hbm,
            smem,
            hbm,
            hbm,
            vmem,
        ],
        out_specs=hbm,
        out_shape=jax.ShapeDtypeStruct((half, ROWS, LANES), bf16),
        scratch_shapes=[
            pltpu.SMEM((devices, LANES), jnp.int32),
            pltpu.SemaphoreType.DMA,
            pltpu.VMEM((levels, levels), bf16),
            pltpu.SemaphoreType.DMA,
            pltpu.VMEM((padded, rows - LANES), bf16),
            pltpu.VMEM((rows, split), bf16),
            pltpu.VMEM((rows, width - split), bf16),
            pltpu.SemaphoreType.DMA((len(parts),)),
            pltpu.VMEM((half, ROWS, LANES), bf16),
            pltpu.SemaphoreType.DMA((PARTS,)),
        ]
        + scratch,
        compiler_params=params(56),
        name="right_side",
    )(index, held_orders, state, height_operator, pressure_column)

    arrived = lax.all_to_all(
        message.reshape(devices, pair_count * ROWS, LANES), GRP_WAVE, 0, 0, tiled=True
    ).reshape(devices, pair_count, ROWS, LANES)

    depth = -(-(LANES + (levels - LANES) * (2 * slot_count + 1)) // 16) * 16
    weights = jnp.einsum("al,jtkl->jtak", table[:depth], inverses, preferred_element_type=f32)
    weights = jnp.einsum("jtak,bk->jtab", weights.astype(bf16), table, preferred_element_type=f32)
    weights = weights.astype(bf16)
    words = index[:, :WORDS].reshape(-1)
    chunk = 32
    solved = pl.pallas_call(
        functools.partial(solve_kernel, (levels, slot_count, chunk)),
        in_specs=[smem, smem, vmem, vmem],
        out_specs=hbm,
        out_shape=jax.ShapeDtypeStruct((devices, pair_count, ROWS, LANES), bf16),
        scratch_shapes=[
            pltpu.VMEM((devices, pair_count, ROWS, LANES), bf16),
            pltpu.SemaphoreType.DMA((PARTS,)),
        ],
        compiler_params=params(24),
        name="solve",
    )(pair_lows, words, arrived, weights)

    returned = lax.all_to_all(
        solved.reshape(devices, pair_count * ROWS, LANES), GRP_WAVE, 0, 0, tiled=True
    ).reshape(half, ROWS, LANES)

    head = levels // 8 * 8
    response = jnp.concatenate(
        [jnp.eye(levels, dtype=bf16), -thermal_response_matrix, -mass_row[None, :]], axis=0
    )
    response = jnp.dot(response, table.T, preferred_element_type=f32).astype(bf16)
    return pl.pallas_call(
        functools.partial(final_kernel, (levels, slot_count, slot_width, truncation, pair_count)),
        in_specs=[smem, smem, vmem, hbm, vmem],
        out_specs=hbm,
        out_shape=jax.ShapeDtypeStruct((rows, width), bf16),
        scratch_shapes=[
            pltpu.VMEM((rows - head, split), bf16),
            pltpu.VMEM((rows - head, width - split), bf16),
            pltpu.SemaphoreType.DMA((len(parts),)),
            pltpu.VMEM((rows, split), bf16),
            pltpu.VMEM((rows, width - split), bf16),
            pltpu.SemaphoreType.DMA((len(parts),)),
        ]
        + scratch,
        compiler_params=params(48),
        name="final",
    )(words, held_orders, returned, state, response)


def solution(mesh):
    torus = Mesh(
        mesh.devices.reshape(mesh.shape["grp"], 4, 4, 2), ("grp", "wave_0", "wave_1", "wave_2")
    )
    placed = (
        P(None, GRP_WAVE),
        P(GRP_WAVE),
        P(GRP_WAVE),
        P(GRP_WAVE, None, None, None),
        P(),
        P(),
        P(),
        P(),
    )
    return jax.shard_map(
        shards, mesh=torus, in_specs=placed, out_specs=P(None, GRP_WAVE), check_vma=False
    )
```

```python
import functools

import jax
import jax.numpy as jnp
import numpy as np
from jax import lax
from jax.experimental import pallas as pl
from jax.experimental.pallas import tpu as pltpu
from jax.sharding import Mesh
from jax.sharding import PartitionSpec as P

GRP_WAVE = ("grp", "wave_0", "wave_1", "wave_2")

LANES = 128
ROWS = 24
FRONT = 768
WORDS = 8
TILE = 3840
LAST_TILE = 3072
PARTS = 4
BIG = 1 << 20
LOW = 17
UP = 25


def edge_masks(slot_count, edge, shape, row_dim):
    rows = lax.broadcasted_iota(jnp.int32, shape, row_dim)
    lanes = lax.broadcasted_iota(jnp.int32, shape, len(shape) - 1)
    group = rows // 2
    return (lanes >= edge * group) & (lanes < edge * (group + 1)) & (rows < 4 * slot_count + 2)


def parity_fold(parts, axis):
    total = parts[0]
    for part in parts[1:]:
        total = total + part
    total = total + pltpu.roll(total, 2, axis)
    return total + pltpu.roll(total, 4, axis)


def slot_lines(columns, orders_ref, slot_count, slot_width):
    order = jnp.full(columns.shape, -1, jnp.int32)
    place = columns
    for s in range(slot_count):
        inside = (columns >= s * slot_width) & (columns < (s + 1) * slot_width)
        order = jnp.where(inside, orders_ref[s], order)
        place = jnp.where(inside, columns - s * slot_width, place)
    return order, place // 2


def column_parts(width, tile):
    starts = list(range(0, width - tile // 2, tile))
    return [(a, b - a) for a, b in zip(starts, starts[1:] + [width])]


def state_copies(state_ref, first, body, tail, sems, tile):
    copies = []
    parts = column_parts(state_ref.shape[1], tile)
    for k, (start, size) in enumerate(parts):
        source = state_ref.at[pl.ds(first, body.shape[0]), pl.ds(start, size)]
        target = tail if k == len(parts) - 1 else body.at[:, pl.ds(start, size)]
        copies.append(pltpu.make_async_copy(source, target, sems.at[k]))
    return copies


def rhs_kernel(
    sizes,
    index_ref,
    orders_ref,
    state_ref,
    height_ref,
    pressure_ref,
    out_ref,
    near,
    index_sem,
    height,
    height_sem,
    drive,
    body,
    tail,
    state_sems,
    stage,
    out_sems,
    xm,
    xe,
    lm,
    le,
    um,
    ue,
):
    levels, slot_count, slot_width, truncation, pair_count = sizes
    half = (truncation + 1) // 2
    parts = column_parts(state_ref.shape[1], TILE)
    bring = pltpu.make_async_copy(height_ref, height, height_sem)
    bring.start()
    copies = state_copies(state_ref, 0, body, tail, state_sems, TILE)
    for copy in copies:
        copy.start()
    fetch = pltpu.make_async_copy(index_ref, near, index_sem)
    fetch.start()

    edge_count = levels - LANES
    lane = lax.broadcasted_iota(jnp.int32, (LANES, drive.shape[0] - LANES), 0)
    group = jnp.zeros_like(lane)
    for g in range(1, 2 * slot_count + 2):
        group = group + jnp.where(lane >= edge_count * g, 1, 0)
    wanted = lax.broadcasted_iota(jnp.int32, lane.shape, 1) == lane - edge_count * group
    spread = jnp.where(wanted & (group <= 2 * slot_count), 1.0, 0.0).astype(jnp.bfloat16)
    column = jnp.broadcast_to(pressure_ref[...].reshape(1, levels).astype(jnp.float32), (8, levels))
    column = jnp.transpose(column)[:, :1]
    drive[...] = jnp.zeros_like(drive)
    last = drive.shape[1] - 1
    drive[:levels, last:] = column.astype(jnp.bfloat16)
    bring.wait()
    drive[:levels, last - levels : last] = height[...]
    padded = drive.shape[0]

    for k, (start, size) in enumerate(parts):
        copies[k].wait()
        if k == len(parts) - 1:
            upper, lower = tail[:padded, :], tail[LANES:, :]
        else:
            upper = body[:padded, start : start + size]
            lower = body[LANES:, start : start + size]
        columns = start + lax.broadcasted_iota(jnp.int32, (1, size), 1)
        order, coeff = slot_lines(columns, orders_ref, slot_count, slot_width)
        degree = jnp.where(coeff <= truncation - order, order + coeff, coeff - 1)
        lap = (degree * (degree + 1)).astype(jnp.float32) / float(truncation * (truncation + 1))
        pull = jnp.dot(drive[...], lower, preferred_element_type=jnp.float32)
        right = (upper.astype(jnp.float32) + lap * pull).astype(jnp.bfloat16)
        xm[pl.ds(FRONT + start, size), :] = jnp.transpose(right[:LANES].astype(jnp.float32))
        xe[pl.ds(FRONT + start, size), :] = lax.dot_general(
            jnp.transpose(right[LANES:].astype(jnp.float32)).astype(jnp.bfloat16),
            spread,
            (((1,), (1,)), ((), ())),
            preferred_element_type=jnp.float32,
        )

    def regroup(s, carry):
        order = jnp.maximum(orders_ref[s], 0)
        base = FRONT + s * slot_width
        for p in range(2):
            for x, low, up in ((xm, lm, um), (xe, le, ue)):
                up[pl.ds(2 * s + p, half, stride=UP), :] = x[
                    pl.ds(base + 2 * (half + 1) + p, half, stride=2), :
                ]
                low[pl.ds(2 * s + p, half, stride=LOW), :] = x[
                    pl.ds(base - 2 * order + p, half, stride=2), :
                ]
                up[pl.ds(2 * (slot_count + s) + p, half, stride=UP), :] = x[
                    pl.ds(base + 2 * (half - order) + p, half, stride=2), :
                ]

                @pl.when(orders_ref[s] >= 0)
                def _(x=x, up=up, p=p):
                    third = UP * (half - 1 - order) + 4 * slot_count + p
                    up[pl.ds(third, 1), :] = x[
                        pl.ds(base + 2 * (truncation + 1 - order) + p, 1), :
                    ]

        return carry

    lax.fori_loop(0, slot_count, regroup, 0)

    row = lax.broadcasted_iota(jnp.int32, (16, LANES), 0)
    order_rows = jnp.full((16, LANES), BIG, jnp.int32)
    for s in range(slot_count):
        order_rows = jnp.where(row // 2 == s, jnp.maximum(orders_ref[s], 0), order_rows)
    mask = edge_masks(slot_count, levels - LANES, (ROWS, LANES), 0)
    bottom = lax.broadcasted_iota(jnp.int32, (8, LANES), 0) >= 6

    def assemble(d, j):
        n = near[d, j]
        start = UP * (half - 1 - n)
        low = LOW * n
        lines = um[pl.ds(start, ROWS), :]
        edge = ue[pl.ds(start, ROWS), :]
        own = order_rows <= n
        top = jnp.where(own, lm[pl.ds(low, 16), :], lines[:16])
        top_edge = jnp.where(own, le[pl.ds(low, 16), :], edge[:16])
        folded = parity_fold(
            [
                jnp.where(mask[:8], top_edge[:8], 0.0),
                jnp.where(mask[8:16], top_edge[8:], 0.0),
                jnp.where(mask[16:], edge[16:], 0.0),
            ],
            0,
        )
        block = jnp.concatenate([top, jnp.where(bottom, folded, lines[16:])], axis=0)
        stage[d * pair_count + j] = block.astype(jnp.bfloat16)

    fetch.wait()
    count = half // pair_count // PARTS
    sends = []
    for k in range(PARTS):

        def assemble_all(d, carry):
            for j in range(pair_count):
                assemble(d, j)
            return carry

        lax.fori_loop(k * count, (k + 1) * count, assemble_all, 0, unroll=4)
        some = pl.ds(k * count * pair_count, count * pair_count)
        sends.append(pltpu.make_async_copy(stage.at[some], out_ref.at[some], out_sems.at[k]))
        sends[-1].start()
    for send in sends:
        send.wait()


def solve_kernel(
    sizes, lows_ref, index_ref, blocks_ref, weights_ref, out_ref, stage, out_sems
):
    levels, slot_count, chunk = sizes
    devices, pair_count = blocks_ref.shape[0], blocks_ref.shape[1]
    shape = (chunk, ROWS, LANES)
    mask = edge_masks(slot_count, levels - LANES, shape, 1)
    row = lax.broadcasted_iota(jnp.int32, shape, 1)
    slot = lax.broadcasted_iota(jnp.int32, (16, LANES), 0) // 2
    depth = weights_ref.shape[2]
    empty = jnp.zeros((2 * LANES - depth, 2 * LANES), jnp.bfloat16)

    def whole(j, t):
        return jnp.concatenate([weights_ref[j, t], empty], axis=0)

    def solve_some(first):
        orders = []
        for k in range(chunk):
            lines = jnp.full((16, LANES), BIG, jnp.int32)
            for s in range(slot_count):
                order = index_ref[(first + k) * WORDS + pair_count + s]
                lines = jnp.where(slot == s, order, lines)
            orders.append(lines)
        orders = jnp.stack(orders)
        here = pl.ds(first, chunk)
        for j in range(pair_count):
            body = blocks_ref[here, j].astype(jnp.float32)
            edge = jnp.where(row % 2 == 0, body[:, ROWS - 2 : ROWS - 1], body[:, ROWS - 1 :])
            edge = jnp.where(mask, edge, 0.0)
            lines = jnp.concatenate([body, edge], axis=-1)
            top = lines[:, :16].reshape(chunk * 16, 2 * LANES).astype(jnp.bfloat16)
            lines = lines.reshape(chunk * ROWS, 2 * LANES).astype(jnp.bfloat16)
            upper = jnp.dot(lines, whole(j, 1), preferred_element_type=jnp.float32)
            upper = upper.reshape(chunk, ROWS, 2 * LANES)
            lower = jnp.dot(top, whole(j, 0), preferred_element_type=jnp.float32)
            lower = lower.reshape(chunk, 16, 2 * LANES)
            own = orders <= lows_ref[j]
            main = jnp.where(own, lower[..., :LANES], upper[:, :16, :LANES])
            edge = jnp.where(own, lower[..., LANES:], upper[:, :16, LANES:])
            edge = jnp.where(mask[:, :16], edge, 0.0)
            rest = jnp.where(mask[:, 16:], upper[:, 16:, LANES:], 0.0)
            folded = parity_fold([edge[:, :8], edge[:, 8:], rest], 1)
            rest = jnp.where(row[:, 16:] >= ROWS - 2, folded, upper[:, 16:, :LANES])
            stage[here, j] = jnp.concatenate([main, rest], axis=1).astype(jnp.bfloat16)

    count = devices // PARTS
    sends = []
    for k in range(PARTS):

        def solve_all(c, carry):
            solve_some(k * count + c * chunk)
            return carry

        lax.fori_loop(0, count // chunk, solve_all, 0)
        some = pl.ds(k * count, count)
        sends.append(pltpu.make_async_copy(stage.at[some], out_ref.at[some], out_sems.at[k]))
        sends[-1].start()
    for send in sends:
        send.wait()


def final_kernel(
    sizes,
    index_ref,
    orders_ref,
    blocks_ref,
    state_ref,
    weights_ref,
    out_ref,
    body,
    tail,
    state_sems,
    out_body,
    out_tail,
    out_sems,
    xm,
    xe,
    lm,
    le,
    um,
    ue,
):
    levels, slot_count, slot_width, truncation, pair_count = sizes
    half = (truncation + 1) // 2
    parts = column_parts(state_ref.shape[1], LAST_TILE)
    head = state_ref.shape[0] - body.shape[0]
    copies = state_copies(state_ref, head, body, tail, state_sems, LAST_TILE)
    for copy in copies:
        copy.start()

    mask = edge_masks(slot_count, levels - LANES, (ROWS, LANES), 0)
    even = lax.broadcasted_iota(jnp.int32, (ROWS, LANES), 0) % 2 == 0

    def unfold(d, carry):
        for j in range(pair_count):
            n = index_ref[d * WORDS + j]
            block = blocks_ref[d * pair_count + j].astype(jnp.float32)
            edge = jnp.where(even, block[ROWS - 2 : ROWS - 1], block[ROWS - 1 :])
            edge = jnp.where(mask, edge, 0.0)
            start = UP * (half - 1 - n)
            low = LOW * n
            um[pl.ds(start, ROWS), :] = block
            ue[pl.ds(start, ROWS), :] = edge
            lm[pl.ds(low, 16), :] = block[:16]
            le[pl.ds(low, 16), :] = edge[:16]
        return carry

    lax.fori_loop(0, half // pair_count, unfold, 0, unroll=4)

    def regroup(k, carry):
        s = slot_count - 1 - k
        order = jnp.maximum(orders_ref[s], 0)
        base = FRONT + s * slot_width
        for p in range(2):
            for x, low, up in ((xm, lm, um), (xe, le, ue)):
                x[pl.ds(base + 2 * (half + 1) + p, half, stride=2), :] = up[
                    pl.ds(2 * s + p, half, stride=UP), :
                ]
                x[pl.ds(base - 2 * order + p, half, stride=2), :] = low[
                    pl.ds(2 * s + p, half, stride=LOW), :
                ]
                x[pl.ds(base + 2 * (half - order) + p, half, stride=2), :] = up[
                    pl.ds(2 * (slot_count + s) + p, half, stride=UP), :
                ]
            third = UP * (half - 1 - order) + 4 * slot_count + p
            place = base + 2 * (truncation + 1 - order) + p
            xm[pl.ds(place, 1), :] = um[pl.ds(third, 1), :]
            xe[pl.ds(place, 1), :] = ue[pl.ds(third, 1), :]
        return carry

    lax.fori_loop(0, slot_count, regroup, 0)

    row = lax.broadcasted_iota(jnp.int32, (state_ref.shape[0] - head, 1), 0)
    sends = []
    for k, (start, size) in enumerate(parts):
        copies[k].wait()
        at_end = k == len(parts) - 1
        base = tail[...] if at_end else body[:, start : start + size]
        lines = [x[pl.ds(FRONT + start, size), :] for x in (xm, xe)]
        moved = lax.dot_general(
            weights_ref[...],
            jnp.concatenate(lines, axis=1).astype(jnp.bfloat16),
            (((1,), (1,)), ((), ())),
            preferred_element_type=jnp.float32,
        )
        columns = start + lax.broadcasted_iota(jnp.int32, (1, size), 1)
        order, _ = slot_lines(columns, orders_ref, slot_count, slot_width)
        live = order >= 0
        kept = jnp.where(row >= levels - head, base.astype(jnp.float32), 0.0)
        first = jnp.where(live, moved[:head], 0.0).astype(jnp.bfloat16)
        second = jnp.where(live, kept + moved[head:], 0.0).astype(jnp.bfloat16)
        if at_end:
            out_tail[:head, :] = first
            out_tail[head:, :] = second
            source = out_tail
        else:
            out_body[:head, start : start + size] = first
            out_body[head:, start : start + size] = second
            source = out_body.at[:, pl.ds(start, size)]
        target = out_ref.at[:, pl.ds(start, size)]
        sends.append(pltpu.make_async_copy(source, target, out_sems.at[k]))
        sends[-1].start()
    for send in sends:
        send.wait()


def level_of_lane(levels, slot_count):
    edge = levels - LANES
    table = np.zeros((2 * LANES, levels), np.float32)
    table[np.arange(LANES), np.arange(LANES)] = 1.0
    folded = np.arange(edge * (2 * slot_count + 1))
    table[LANES + folded, LANES + folded % edge] = 1.0
    return table


def shards(
    state,
    held_orders,
    pair_lows,
    inverses,
    height_operator,
    pressure_column,
    thermal_response_matrix,
    mass_row,
):
    levels = height_operator.shape[0]
    pair_count = pair_lows.shape[0]
    slot_count = held_orders.shape[0]
    devices = lax.axis_size(GRP_WAVE)
    half = pair_count * devices
    truncation = 2 * half - 1
    slot_width = 2 * (truncation + 2)
    width = slot_count * slot_width
    rows = state.shape[0]
    parts = column_parts(width, TILE)
    split = parts[-1][0]
    last_parts = column_parts(width, LAST_TILE)
    last_split = last_parts[-1][0]
    bf16, f32 = jnp.bfloat16, jnp.float32
    vmem = pl.BlockSpec(memory_space=pltpu.VMEM)
    smem = pl.BlockSpec(memory_space=pltpu.SMEM)
    hbm = pl.BlockSpec(memory_space=pl.ANY)

    def params(mib):
        return pltpu.CompilerParams(vmem_limit_bytes=mib * 1024 * 1024)

    scratch = [
        pltpu.VMEM((FRONT + width + 6, LANES), f32),
        pltpu.VMEM((FRONT + width + 6, LANES), f32),
        pltpu.VMEM((LOW * half, LANES), f32),
        pltpu.VMEM((LOW * half, LANES), f32),
        pltpu.VMEM((UP * half, LANES), f32),
        pltpu.VMEM((UP * half, LANES), f32),
    ]

    own = jnp.concatenate([pair_lows, held_orders])
    own = jnp.pad(own, (0, LANES - own.shape[0]))
    index = lax.all_to_all(
        jnp.broadcast_to(own[None, None], (devices, 1, LANES)), GRP_WAVE, 0, 0, tiled=True
    ).reshape(devices, LANES)

    table = level_of_lane(levels, slot_count)
    padded = -(-levels // 16) * 16
    table = jnp.asarray(table, bf16)

    message = pl.pallas_call(
        functools.partial(rhs_kernel, (levels, slot_count, slot_width, truncation, pair_count)),
        in_specs=[
            hbm,
            smem,
            hbm,
            hbm,
            vmem,
        ],
        out_specs=hbm,
        out_shape=jax.ShapeDtypeStruct((half, ROWS, LANES), bf16),
        scratch_shapes=[
            pltpu.SMEM((devices, LANES), jnp.int32),
            pltpu.SemaphoreType.DMA,
            pltpu.VMEM((levels, levels), bf16),
            pltpu.SemaphoreType.DMA,
            pltpu.VMEM((padded, rows - LANES), bf16),
            pltpu.VMEM((rows, split), bf16),
            pltpu.VMEM((rows, width - split), bf16),
            pltpu.SemaphoreType.DMA((len(parts),)),
            pltpu.VMEM((half, ROWS, LANES), bf16),
            pltpu.SemaphoreType.DMA((PARTS,)),
        ]
        + scratch,
        compiler_params=params(56),
        name="right_side",
    )(index, held_orders, state, height_operator, pressure_column)

    arrived = lax.all_to_all(
        message.reshape(devices, pair_count * ROWS, LANES), GRP_WAVE, 0, 0, tiled=True
    ).reshape(devices, pair_count, ROWS, LANES)

    depth = -(-(LANES + (levels - LANES) * (2 * slot_count + 1)) // 16) * 16
    weights = jnp.einsum("al,jtkl->jtak", table[:depth], inverses, preferred_element_type=f32)
    weights = jnp.einsum("jtak,bk->jtab", weights.astype(bf16), table, preferred_element_type=f32)
    weights = weights.astype(bf16)
    words = index[:, :WORDS].reshape(-1)
    chunk = 32
    solved = pl.pallas_call(
        functools.partial(solve_kernel, (levels, slot_count, chunk)),
        in_specs=[smem, smem, vmem, vmem],
        out_specs=hbm,
        out_shape=jax.ShapeDtypeStruct((devices, pair_count, ROWS, LANES), bf16),
        scratch_shapes=[
            pltpu.VMEM((devices, pair_count, ROWS, LANES), bf16),
            pltpu.SemaphoreType.DMA((PARTS,)),
        ],
        compiler_params=params(24),
        name="solve",
    )(pair_lows, words, arrived, weights)

    returned = lax.all_to_all(
        solved.reshape(devices, pair_count * ROWS, LANES), GRP_WAVE, 0, 0, tiled=True
    ).reshape(half, ROWS, LANES)

    head = levels // 8 * 8
    response = jnp.concatenate(
        [jnp.eye(levels, dtype=bf16), -thermal_response_matrix, -mass_row[None, :]], axis=0
    )
    response = jnp.dot(response, table.T, preferred_element_type=f32).astype(bf16)
    return pl.pallas_call(
        functools.partial(final_kernel, (levels, slot_count, slot_width, truncation, pair_count)),
        in_specs=[smem, smem, vmem, hbm, vmem],
        out_specs=hbm,
        out_shape=jax.ShapeDtypeStruct((rows, width), bf16),
        scratch_shapes=[
            pltpu.VMEM((rows - head, last_split), bf16),
            pltpu.VMEM((rows - head, width - last_split), bf16),
            pltpu.SemaphoreType.DMA((len(last_parts),)),
            pltpu.VMEM((rows, last_split), bf16),
            pltpu.VMEM((rows, width - last_split), bf16),
            pltpu.SemaphoreType.DMA((len(last_parts),)),
        ]
        + scratch,
        compiler_params=params(48),
        name="final",
    )(words, held_orders, returned, state, response)


def solution(mesh):
    torus = Mesh(
        mesh.devices.reshape(mesh.shape["grp"], 4, 4, 2), ("grp", "wave_0", "wave_1", "wave_2")
    )
    placed = (
        P(None, GRP_WAVE),
        P(GRP_WAVE),
        P(GRP_WAVE),
        P(GRP_WAVE, None, None, None),
        P(),
        P(),
        P(),
        P(),
    )
    return jax.shard_map(
        shards, mesh=torus, in_specs=placed, out_specs=P(None, GRP_WAVE), check_vma=False
    )
```
